32 devices in a mesh: group: 8 (over y, x, core), shard: 4 (over z).
Axes of the slice: x: 2, y: 2, z: 4, core: 2. Of those that a mesh axis runs over, the one named last changes fastest.
Arguments:
- momentum: bfloat16 [8, 7168, 2048], P(None, ('group', 'shard'))
- gradient: bfloat16 [8, 7168, 2048], P(None, ('group', 'shard'))
- q_prev: bfloat16 [8, 3, 2048, 128], P('group', None, 'shard'), may hold values from -6 to 6
- owner_group: int32 [8], replicated, may hold values from 0 to 7, as said below
- group_counts: int32 [8], replicated, may hold values from 0 to 3, as said below
Outputs:
- momentum_next: bfloat16 [8, 7168, 2048], P(None, ('group', 'shard'))
- update: bfloat16 [8, 7168, 2048], P(None, ('group', 'shard'))
- q_next: bfloat16 [8, 3, 2048, 128], P('group', None, 'shard')
The draws below stay inside these ranges and needn't reach their ends.
Inputs may be any that keep to these rules, and one draw needn't show every extreme that they name: `owner_group`: each group owns at most 3 experts and some group owns exactly 3; a group's experts fill its slots 0, 1, ... in increasing expert order. `group_counts`: entry g is the number of experts whose owner_group is g, except for one or two groups that own some experts, where it is one less; it equals 3 for some group that owns 3 experts.
All inputs are finite; a program needn't handle non-finite values.
Results may differ from the reference program's by a relative error of at most 0.0059.
Values may be sent and summed in bfloat16 or wider, within the bound.
A program may use at most 128 MiB of HBM per device.

```python
import math
import jax
import jax.numpy as jnp
from jax import lax

D = 7168
H = 2048
RANK = 128
EXPERTS = 8
CAP = 3
BLOCK = 224
N_GROUP = 8
N_SHARD = 4


def entry_scales(key):
    rows = jnp.arange(D, dtype=jnp.int32)
    position = (rows // BLOCK % N_SHARD).astype(jnp.float32) / max(N_SHARD - 1, 1)
    rising = jnp.exp(math.log(3.0) * (position - 0.5))
    row_scale = jnp.exp(jax.random.uniform(jax.random.fold_in(key, 21), (EXPERTS, D, 1), jnp.float32, math.log(0.3), math.log(3.0)))
    col_scale = jnp.exp(jax.random.uniform(jax.random.fold_in(key, 22), (EXPERTS, 1, H), jnp.float32, math.log(0.3), math.log(3.0)))
    return row_scale * rising[None, :, None] * col_scale


def shared_part(key):
    left_factor = jax.random.normal(jax.random.fold_in(key, 41), (EXPERTS, D, RANK), jnp.float32)
    right_factor = jax.random.normal(jax.random.fold_in(key, 42), (EXPERTS, RANK, H), jnp.float32)
    return jnp.einsum('edk,ekh->edh', left_factor, right_factor) / math.sqrt(RANK)


def noise_part(key, salt):
    base = jax.random.fold_in(key, salt)
    values = jax.random.normal(base, (EXPERTS, D, H), jnp.float32)
    return values


def entries(key, salt):
    mixed = 0.894 * shared_part(key) + 0.447 * noise_part(key, salt)
    return mixed * entry_scales(key)


def draw_momentum(key, part):
    return entries(key, 31).astype(jnp.bfloat16)


def draw_gradient(key, part):
    return (0.5 * entries(key, 32)).astype(jnp.bfloat16)


def owner_plan(key):
    total_slots = N_GROUP * CAP
    full_group = jax.random.randint(jax.random.fold_in(key, 12), (), 0, N_GROUP)
    slot_ids = jnp.arange(total_slots, dtype=jnp.int32)
    scores = jax.random.randint(jax.random.fold_in(key, 11), (total_slots,), 0, 2 ** 20) * total_slots + slot_ids
    scores = jnp.where(slot_ids // CAP == full_group, scores + 2 ** 30, scores)
    forced_groups = jnp.array([N_GROUP // 2, 0, 3], dtype=jnp.int32)
    forced_slots = forced_groups * CAP
    mandated_reward = jnp.array([2, 1, 0], dtype=jnp.int32)
    mandated_flag = slot_ids[:, None] == forced_slots[None, :]
    mandated_rating = 2 ** 30 + 2 ** 29 + jnp.sum(jnp.where(mandated_flag, mandated_reward[None, :], 0), axis=1)
    scores = jnp.where(jnp.any(mandated_flag, axis=1), mandated_rating, scores).astype(jnp.int32)
    picked_scores, chosen = lax.top_k(scores, EXPERTS)
    chosen_group = (chosen // CAP).astype(jnp.int32)
    shuffle = jax.random.permutation(jax.random.fold_in(key, 13), EXPERTS - 3)
    owner = jnp.concatenate([chosen_group[:3], chosen_group[3:][shuffle]]).astype(jnp.int32)
    group_ids = jnp.arange(N_GROUP, dtype=jnp.int32)
    counts = jnp.sum((owner[None, :] == group_ids[:, None]).astype(jnp.int32), axis=1).astype(jnp.int32)
    holds_forced = jnp.any(group_ids[:, None] == forced_groups[None, :], axis=1)
    eligible = (counts >= 1) & (group_ids != full_group) & jnp.logical_not(holds_forced & (counts < 2))
    group_scores = jax.random.randint(jax.random.fold_in(key, 14), (N_GROUP,), 0, 2 ** 20) * N_GROUP + group_ids
    group_scores = jnp.where(eligible, group_scores + 2 ** 26, group_scores)
    top_scores, picked = lax.top_k(group_scores, 2)
    short = jnp.any(group_ids[:, None] == picked[None, :], axis=1) & eligible
    counts = (counts - short.astype(jnp.int32)).astype(jnp.int32)
    return (owner, counts)


def draw_owner_group(key, part):
    return owner_plan(key)[0]


def draw_group_counts(key, part):
    return owner_plan(key)[1]


def levels(key, dims, split, low, top_value):
    loudness, own = 1.0, jax.random.fold_in(key, 6)
    for axis_at, parts in split:
        heights = jnp.exp(jax.random.uniform(jax.random.fold_in(own, axis_at), (parts,), jnp.float32, low / len(split), top_value / len(split)))
        loudness = loudness * jnp.repeat(heights, dims[axis_at] // parts).reshape([-1 if axis == axis_at else 1 for axis in range(len(dims))])
    return loudness


def gaussian(own_key, shape, deviation, limit, shards=(), kind=jnp.bfloat16):
    gain = levels(own_key, shape, shards, -0.22, 0.18) if shards else 1.0
    values = jax.random.normal(own_key, shape, jnp.float32) * deviation * gain
    return jnp.minimum(jnp.maximum(values, -limit), limit).astype(kind)


def setup_inputs(seed: int = 0) -> dict:
    streams_of = jax.random.split(jax.random.key(seed), 6)
    return {
        "momentum": draw_momentum(jax.random.fold_in(streams_of[5], 71), 0),
        "gradient": draw_gradient(jax.random.fold_in(streams_of[5], 71), 0),
        "q_prev": gaussian(streams_of[2], (N_GROUP, CAP, H, RANK), 1.0, 6.0, ((0, 8), (2, 4))),
        "owner_group": draw_owner_group(jax.random.fold_in(streams_of[5], 71), 0),
        "group_counts": draw_group_counts(jax.random.fold_in(streams_of[5], 71), 0),
    }


stability_offset = 1e-06
momentum_decay = 0.6

def owner_slots(owner_group):
    experts = owner_group.shape[0]
    expert_ids = jnp.arange(experts, dtype=jnp.int32)
    same_owner = owner_group[:, None] == owner_group[None, :]
    earlier = expert_ids[None, :] < expert_ids[:, None]
    return lax.optimization_barrier(jnp.sum((same_owner & earlier).astype(jnp.int32), axis=1)).astype(jnp.int32)

def reference(momentum, gradient, q_prev, owner_group, group_counts):
    slot_of = owner_slots(owner_group)
    keep = slot_of < group_counts[owner_group]
    q_each = q_prev[owner_group, slot_of]
    update_multiplier = math.sqrt(D / RANK)

    def one_expert(items):
        moment_one, grad_one, q_one, keep_one = items
        combined = (moment_one.astype(jnp.float32) + grad_one.astype(jnp.float32)).astype(jnp.bfloat16)
        q_used = jnp.where(keep_one, q_one, jnp.zeros_like(q_one))
        unnormalized_basis = jnp.dot(combined, q_used, preferred_element_type=jnp.float32)
        left_unit = (unnormalized_basis * lax.rsqrt(lax.optimization_barrier(jnp.sum(unnormalized_basis * unnormalized_basis, axis=0)) + stability_offset)[None, :]).astype(jnp.bfloat16)
        right = jnp.dot(combined.T, left_unit, preferred_element_type=jnp.float32)
        q_new = (right * lax.rsqrt(lax.optimization_barrier(jnp.mean(right * right, axis=0)) + stability_offset)[None, :]).astype(jnp.bfloat16)
        update_one = (jnp.dot(left_unit, q_new.T, preferred_element_type=jnp.float32) * update_multiplier).astype(jnp.bfloat16)
        low_rank = jnp.dot(left_unit, right.astype(jnp.bfloat16).T, preferred_element_type=jnp.float32)
        moment_next = (combined.astype(jnp.float32) - (1.0 - momentum_decay) * low_rank).astype(jnp.bfloat16)
        return (moment_next, update_one, jnp.where(keep_one, q_new, jnp.zeros_like(q_new)))
    velocity_states, update_list, q_all = lax.map(one_expert, (momentum, gradient, q_each, keep))
    q_next = jnp.zeros_like(q_prev).at[owner_group, slot_of].set(q_all)
    return (velocity_states, update_list, q_next)
```

```python
import math

import jax
import jax.numpy as jnp
from jax import lax
from jax.experimental import pallas as pl
from jax.experimental.pallas import tpu as pltpu
from jax.sharding import PartitionSpec as P

D = 7168
RANK = 128

stability_offset = 1e-06
momentum_decay = 0.6
AXES = ("group", "shard")
LANES = 128
F32, BF16 = jnp.float32, jnp.bfloat16


def scalar_slot(owner_ref, e, experts, cap):
    own = owner_ref[e]
    slot = jnp.int32(0)
    for other in range(experts):
        hit = (owner_ref[other] == own) & (other < e)
        slot = slot + jnp.where(hit, 1, 0)
    return own, slot, jnp.minimum(slot, cap - 1)


def exchange(momentum, gradient, q_prev, owner_group, group_counts):
    experts, block, hidden = momentum.shape
    cap, share, rank = q_prev.shape[1:]
    groups, nz = lax.axis_size("group"), lax.axis_size("shard")
    m = groups // 2
    a = 2 ** ((m.bit_length() - 1) // 2)
    b = m // a
    rb = share // groups
    hb = hidden // LANES
    L = hb // m
    L2 = L // 2
    half = rank // 2
    subs = nz // L
    nr = half // subs
    q_view = q_prev.reshape(cap, 2, m, rb, rank)

    counts = [
        ("qcore", 1), ("qplane", m - 1), ("qz", nz - 1), ("qxy", a + b - 2),
        ("qdiag", 2 * (a - 1) * (b - 1)), ("qback", 1),
        ("s1", groups - 1), ("s2", nz - 1),
        ("rcore", 1), ("p1", a + b - 2), ("p2", a + b - 2), ("rz", nz - 1),
        ("gz", nz - 1), ("gxy", a + b - 2), ("gdiag", 2 * (a - 1) * (b - 1)), ("gback", 1),
    ]
    base, total = {}, 0
    for name, n in counts:
        base[name] = total
        total += n

    def kernel(
        mom, grad, q_in, owner_ref, counts_ref,
        comb_out, left_out, right_out,
        mom_buf, grad_buf, comb, q_own, qp, qc_land, qc, qp_land, Q,
        left_raw, left, s1, s1_land, s2, s2_land,
        pt, c_land, cs, p1a, p1b, s2a, s2b, p2a, p2b, ps, z_land, R,
        send, recv, load_sem, q_sem, comb_sem, left_sem, right_sem,
    ):
        g, s = lax.axis_index("group"), lax.axis_index("shard")
        c = lax.rem(g, 2)
        p = g // 2
        y, x = p // b, lax.rem(p, b)
        oc = 1 - c

        def up(v, k, n):
            return lax.rem(v + k, n)

        def down(v, k, n):
            return lax.rem(v + n - k, n)

        def copy(name, e, k, src, dst, device):
            return pltpu.make_async_remote_copy(
                src_ref=src, dst_ref=dst,
                send_sem=send.at[e, base[name] + k], recv_sem=recv.at[e, base[name] + k],
                device_id=device, device_id_type=pl.DeviceIdType.MESH,
            )

        def dev(yy, xx):
            return ((yy * b + xx) * 2 + c, s)

        core = (p * 2 + oc, s)

        def family(name, e):
            out = []
            if name == "qcore":
                out.append((qp.at[e, oc], qc_land.at[e], qc_land.at[e], core))
            elif name == "qplane":
                for k in range(1, m):
                    to = up(p, k, m)
                    out.append((qc.at[e, to], qp_land.at[e, k - 1], qp_land.at[e, k - 1], (to * 2 + c, s)))
            elif name == "qz":
                for k in range(1, nz):
                    here = Q.at[e, c, p, s]
                    out.append((here, here, Q.at[e, c, p, down(s, k, nz)], (g, up(s, k, nz))))
            elif name == "gz":
                def piece(at):
                    rows = pl.ds(pl.multiple_of((at // L) * nr, nr), nr)
                    return R.at[e, c, p * L + lax.rem(at, L), rows]
                for k in range(1, nz):
                    out.append((piece(s), piece(s), piece(down(s, k, nz)), (g, up(s, k, nz))))
            elif name in ("qxy", "gxy"):
                whole = q_place if name == "qxy" else r_place
                for k in range(1, a):
                    out.append((whole(e, y, x), whole(e, y, x), whole(e, down(y, k, a), x), dev(up(y, k, a), x)))
                for k in range(1, b):
                    out.append((whole(e, y, x), whole(e, y, x), whole(e, y, down(x, k, b)), dev(y, up(x, k, b))))
            elif name in ("qdiag", "gdiag"):
                part = q_half if name == "qdiag" else r_half
                for k in range(1, a):
                    for j in range(1, b):
                        xx = down(x, j, b)
                        out.append((part(e, y, xx, 0), part(e, y, xx, 0), part(e, down(y, k, a), xx, 0), dev(up(y, k, a), x)))
                for k in range(1, a):
                    for j in range(1, b):
                        yy = down(y, k, a)
                        out.append((part(e, yy, x, 1), part(e, yy, x, 1), part(e, yy, down(x, j, b), 1), dev(y, up(x, j, b))))
            elif name == "qback":
                out.append((Q.at[e, c], Q.at[e, c], Q.at[e, oc], core))
            elif name == "gback":
                out.append((R.at[e, c], R.at[e, c], R.at[e, oc], core))
            elif name == "s1":
                for k in range(1, groups):
                    out.append((s1.at[e], s1_land.at[e, k - 1], s1_land.at[e, k - 1], (up(g, k, groups), s)))
            elif name == "s2":
                for k in range(1, nz):
                    out.append((s2.at[e], s2_land.at[e, k - 1], s2_land.at[e, k - 1], (g, up(s, k, nz))))
            elif name == "rcore":
                out.append((pt.at[e, oc], c_land.at[e], c_land.at[e], core))
            elif name == "p1":
                for k in range(1, a):
                    out.append((cs.at[e, 0, up(y, k, a)], p1a.at[e, k - 1], p1a.at[e, k - 1], dev(up(y, k, a), x)))
                for k in range(1, b):
                    out.append((cs.at[e, 1, :, up(x, k, b)], p1b.at[e, k - 1], p1b.at[e, k - 1], dev(y, up(x, k, b))))
            elif name == "p2":
                for k in range(1, b):
                    out.append((s2a.at[e, up(x, k, b)], p2a.at[e, k - 1], p2a.at[e, k - 1], dev(y, up(x, k, b))))
                for k in range(1, a):
                    out.append((s2b.at[e, up(y, k, a)], p2b.at[e, k - 1], p2b.at[e, k - 1], dev(up(y, k, a), x)))
            elif name == "rz":
                for k in range(1, nz):
                    at = up(s, k, nz)
                    rows = pl.ds(pl.multiple_of((at // L) * nr, nr), nr)
                    out.append((ps.at[e, lax.rem(at, L), rows], z_land.at[e, k - 1], z_land.at[e, k - 1], (g, at)))
            return out

        def q_place(e, yy, xx):
            return Q.at[e, c, yy * b + xx]

        def q_half(e, yy, xx, h):
            return Q.at[e, c, yy * b + xx, pl.ds(h * (nz // 2), nz // 2)]

        def r_place(e, yy, xx):
            return R.at[e, c, pl.ds((yy * b + xx) * L, L)]

        def r_half(e, yy, xx, h):
            return R.at[e, c, pl.ds((yy * b + xx) * L + h * L2, L2)]

        def start(name, e):
            for k, (src, dst, _, device) in enumerate(family(name, e)):
                copy(name, e, k, src, dst, device).start()

        def arrived(name, e):
            for k, (src, _, dst, device) in enumerate(family(name, e)):
                copy(name, e, k, src, dst, device).wait_recv()

        def sent(name, e):
            for k, (src, dst, _, device) in enumerate(family(name, e)):
                copy(name, e, k, src, dst, device).wait_send()

        def loads(e):
            at = lax.rem(e, 2)
            return (
                pltpu.make_async_copy(mom.at[e], mom_buf.at[at], load_sem.at[at, 0]),
                pltpu.make_async_copy(grad.at[e], grad_buf.at[at], load_sem.at[at, 1]),
            )

        q_load = pltpu.make_async_copy(q_in, q_own, q_sem)
        q_load.start()
        for e in range(min(2, experts)):
            for one in loads(e):
                one.start()

        barrier = pltpu.get_barrier_semaphore()
        for k in range(1, groups):
            pl.semaphore_signal(barrier, inc=1, device_id=(up(g, k, groups), s), device_id_type=pl.DeviceIdType.MESH)
        for k in range(1, nz):
            pl.semaphore_signal(barrier, inc=1, device_id=(g, up(s, k, nz)), device_id_type=pl.DeviceIdType.MESH)

        q_load.wait()

        @pl.loop(0, experts)
        def _(e):
            own, slot, at = scalar_slot(owner_ref, e, experts, cap)
            live = (slot < counts_ref[own]) & (own == g)
            factor = jnp.where(live, 1.0, 0.0).astype(F32)
            for h in range(2):
                qp[e, h] = (q_own[at, h].astype(F32) * factor).astype(BF16)

        pl.semaphore_wait(barrier, groups + nz - 2)

        @pl.loop(0, experts)
        def _(e):
            start("qcore", e)

        def stage_q0(e):
            arrived("qcore", e)
            qc[e] = qp[e, c] + qc_land[e]
            start("qplane", e)

        def stage_q1(e):
            arrived("qplane", e)
            mine = qc[e, p]
            for k in range(m - 1):
                mine = mine + qp_land[e, k]
            Q[e, c, p, s] = mine
            start("qz", e)

        def stage_combine(e):
            for one in loads(e):
                one.wait()
            at = lax.rem(e, 2)
            comb[e] = (mom_buf[at].astype(F32) + grad_buf[at].astype(F32)).astype(BF16)
            pltpu.make_async_copy(comb.at[e], comb_out.at[e], comb_sem.at[e]).start()

            @pl.when(e + 2 < experts)
            def _():
                for one in loads(e + 2):
                    one.start()

        def relay(before, after):
            def stage(e):
                arrived(before, e)
                start(after, e)
            return stage

        def stage_left(e):
            arrived("qback", e)
            acc = jnp.zeros((block, rank), F32)
            span = share // 2
            for z in range(nz):
                for h in range(2):
                    rows = Q[e, h, :, z].reshape(span, rank)
                    lo = z * share + h * span
                    acc = acc + jnp.dot(comb[e, :, lo:lo + span], rows, preferred_element_type=F32)
            left_raw[e] = acc
            s1[e] = jnp.sum(acc * acc, axis=0, keepdims=True)
            start("s1", e)

        def stage_s(e):
            arrived("s1", e)
            tot = s1[e]
            for k in range(groups - 1):
                tot = tot + s1_land[e, k]
            s2[e] = tot
            start("s2", e)

        def stage_part(e):
            arrived("s2", e)
            tot = s2[e]
            for k in range(nz - 1):
                tot = tot + s2_land[e, k]
            unit = left_raw[e] * lax.rsqrt(tot + stability_offset)
            left[e] = unit.astype(BF16)
            pltpu.make_async_copy(left.at[e], left_out.at[e], left_sem.at[e]).start()
            unit_t = unit.T.astype(BF16)
            wide = 2 * LANES
            for j in range(hidden // wide):
                res = jnp.dot(unit_t, comb[e, :, j * wide:(j + 1) * wide], preferred_element_type=F32).astype(BF16)
                for i in range(2):
                    for h in range(2):
                        pt[e, h, 2 * j + i] = res[h * half:(h + 1) * half, i * LANES:(i + 1) * LANES]
            start("rcore", e)

        def stage_chip(e):
            arrived("rcore", e)
            for h in range(2):
                for i in range(L2):
                    for pp in range(m):
                        at = pp * L + h * L2 + i
                        cs[e, h, pp // b, pp % b, i] = (
                            pt[e, c, at].astype(F32) + c_land[e, at].astype(F32)
                        ).astype(BF16)
            start("p1", e)

        def stage_p1(e):
            arrived("p1", e)
            for i in range(b):
                tot = cs[e, 0, y, i].astype(F32)
                for k in range(a - 1):
                    tot = tot + p1a[e, k, i].astype(F32)
                s2a[e, i] = tot.astype(BF16)
            for i in range(a):
                tot = cs[e, 1, i, x].astype(F32)
                for k in range(b - 1):
                    tot = tot + p1b[e, k, i].astype(F32)
                s2b[e, i] = tot.astype(BF16)
            start("p2", e)

        def stage_p2(e):
            arrived("p2", e)
            tot = s2a[e, x].astype(F32)
            for k in range(b - 1):
                tot = tot + p2a[e, k].astype(F32)
            ps[e, 0:L2] = tot.astype(BF16)
            tot = s2b[e, y].astype(F32)
            for k in range(a - 1):
                tot = tot + p2b[e, k].astype(F32)
            ps[e, L2:L] = tot.astype(BF16)
            start("rz", e)

        def stage_rz(e):
            arrived("rz", e)
            rows = pl.ds(pl.multiple_of((s // L) * nr, nr), nr)
            tot = ps[e, lax.rem(s, L), rows].astype(F32)
            for k in range(nz - 1):
                tot = tot + z_land[e, k].astype(F32)
            R[e, c, p * L + lax.rem(s, L), rows] = tot.astype(BF16)
            start("gz", e)

        def stage_done(e):
            arrived("gback", e)
            pltpu.make_async_copy(R.at[e], right_out.at[e], right_sem.at[e]).start()
            for name, _ in counts:
                sent(name, e)

        stages = [
            (0, stage_q0), (1, stage_q1), (2, relay("qz", "qxy")), (3, relay("qxy", "qdiag")),
            (4, relay("qdiag", "qback")), (8, stage_chip), (9, stage_p1), (10, stage_p2),
            (11, stage_rz), (12, relay("gz", "gxy")), (13, relay("gxy", "gdiag")),
            (14, relay("gdiag", "gback")), (6, stage_s), (0, stage_combine), (7, stage_part),
            (5, stage_left), (15, stage_done),
        ]

        @pl.loop(0, experts + 15)
        def _(t):
            for offset, stage in stages:
                @pl.when((t >= offset) & (t < offset + experts))
                def _():
                    stage(t - offset)

        @pl.loop(0, experts)
        def _(e):
            pltpu.make_async_copy(comb.at[e], comb_out.at[e], comb_sem.at[e]).wait()
            pltpu.make_async_copy(left.at[e], left_out.at[e], left_sem.at[e]).wait()
            pltpu.make_async_copy(R.at[e], right_out.at[e], right_sem.at[e]).wait()

    E = experts
    hbm = pl.BlockSpec(memory_space=pl.ANY)
    smem = pl.BlockSpec(memory_space=pltpu.SMEM)
    return pl.pallas_call(
        kernel,
        name="exchange",
        out_shape=(
            jax.ShapeDtypeStruct((E, block, hidden), BF16),
            jax.ShapeDtypeStruct((E, block, rank), BF16),
            jax.ShapeDtypeStruct((E, 2, hb, half, LANES), BF16),
        ),
        in_specs=[hbm, hbm, hbm, smem, smem],
        out_specs=(hbm, hbm, hbm),
        scratch_shapes=[
            pltpu.VMEM((2, block, hidden), BF16),
            pltpu.VMEM((2, block, hidden), BF16),
            pltpu.VMEM((E, block, hidden), BF16),
            pltpu.VMEM((cap, 2, m, rb, rank), BF16),
            pltpu.VMEM((E, 2, m, rb, rank), BF16),
            pltpu.VMEM((E, m, rb, rank), BF16),
            pltpu.VMEM((E, m, rb, rank), BF16),
            pltpu.VMEM((E, m - 1, rb, rank), BF16),
            pltpu.VMEM((E, 2, m, nz, rb, rank), BF16),
            pltpu.VMEM((E, block, rank), F32),
            pltpu.VMEM((E, block, rank), BF16),
            pltpu.VMEM((E, 1, rank), F32),
            pltpu.VMEM((E, groups - 1, 1, rank), F32),
            pltpu.VMEM((E, 1, rank), F32),
            pltpu.VMEM((E, nz - 1, 1, rank), F32),
            pltpu.VMEM((E, 2, hb, half, LANES), BF16),
            pltpu.VMEM((E, hb, half, LANES), BF16),
            pltpu.VMEM((E, 2, a, b, L2, half, LANES), BF16),
            pltpu.VMEM((E, a - 1, b, L2, half, LANES), BF16),
            pltpu.VMEM((E, b - 1, a, L2, half, LANES), BF16),
            pltpu.VMEM((E, b, L2, half, LANES), BF16),
            pltpu.VMEM((E, a, L2, half, LANES), BF16),
            pltpu.VMEM((E, b - 1, L2, half, LANES), BF16),
            pltpu.VMEM((E, a - 1, L2, half, LANES), BF16),
            pltpu.VMEM((E, L, half, LANES), BF16),
            pltpu.VMEM((E, nz - 1, nr, LANES), BF16),
            pltpu.VMEM((E, 2, hb, half, LANES), BF16),
            pltpu.SemaphoreType.DMA((E, total)),
            pltpu.SemaphoreType.DMA((E, total)),
            pltpu.SemaphoreType.DMA((2, 2)),
            pltpu.SemaphoreType.DMA,
            pltpu.SemaphoreType.DMA((E,)),
            pltpu.SemaphoreType.DMA((E,)),
            pltpu.SemaphoreType.DMA((E,)),
        ],
        compiler_params=pltpu.CompilerParams(
            collective_id=0, has_side_effects=True, vmem_limit_bytes=63_000_000
        ),
    )(momentum, gradient, q_view, owner_group, group_counts)


def finish(combined, left, right, owner_group, group_counts, cap, share):
    experts, block, hidden = combined.shape
    rank = left.shape[2]
    hb, half = right.shape[2:4]
    own_blocks = share // LANES

    def kernel(owner_ref, counts_ref, comb, left_ref, right_ref, mom_out, upd_out, q_out, kept):
        e = pl.program_id(0)
        me, s = lax.axis_index("group"), lax.axis_index("shard")

        def block_of(i):
            return jnp.concatenate([right_ref[0, 0, i], right_ref[0, 1, i]], axis=0).astype(F32)

        squares = jnp.zeros((rank, LANES), F32)
        for i in range(hb):
            one = block_of(i)
            squares = squares + one * one
        scale = lax.rsqrt(jnp.sum(squares, axis=1, keepdims=True) / hidden + stability_offset)

        unit = left_ref[0]
        for j in range(hb // 2):
            raw = jnp.concatenate([block_of(2 * j), block_of(2 * j + 1)], axis=1)
            span = slice(2 * j * LANES, (2 * j + 2) * LANES)
            low = jnp.dot(unit, raw.astype(BF16), preferred_element_type=F32)
            mom_out[0, :, span] = (
                comb[0, :, span].astype(F32) - (1.0 - momentum_decay) * low
            ).astype(BF16)
            new = (raw * scale).astype(BF16)
            upd_out[0, :, span] = (
                jnp.dot(unit, new, preferred_element_type=F32) * math.sqrt(D / RANK)
            ).astype(BF16)

        @pl.when(e == 0)
        def _():
            kept[...] = jnp.zeros_like(kept)

        own, slot, at = scalar_slot(owner_ref, e, experts, cap)

        @pl.when((slot < counts_ref[own]) & (own == me))
        def _():
            for i in range(own_blocks):
                kept[at, i] = (block_of(s * own_blocks + i) * scale).astype(BF16).astype(F32)

        @pl.when(e == experts - 1)
        def _():
            for j in range(cap):
                for i in range(own_blocks):
                    q_out[0, j, i * LANES:(i + 1) * LANES, :] = kept[j, i].T.astype(BF16)

    smem = pl.BlockSpec(memory_space=pltpu.SMEM)
    row = pl.BlockSpec((1, block, hidden), lambda e: (e, 0, 0))
    return pl.pallas_call(
        kernel,
        name="finish",
        grid=(experts,),
        out_shape=(
            jax.ShapeDtypeStruct(combined.shape, BF16),
            jax.ShapeDtypeStruct(combined.shape, BF16),
            jax.ShapeDtypeStruct((1, cap, share, rank), BF16),
        ),
        in_specs=[
            smem, smem, row,
            pl.BlockSpec((1, block, rank), lambda e: (e, 0, 0)),
            pl.BlockSpec((1, 2, hb, half, LANES), lambda e: (e, 0, 0, 0, 0)),
        ],
        out_specs=(row, row, pl.BlockSpec((1, cap, share, rank), lambda e: (0, 0, 0, 0))),
        scratch_shapes=[pltpu.VMEM((cap, own_blocks, rank, LANES), F32)],
        compiler_params=pltpu.CompilerParams(dimension_semantics=("arbitrary",)),
    )(owner_group, group_counts, combined, left, right)


def shards(momentum, gradient, q_prev, owner_group, group_counts):
    cap, share = q_prev.shape[1:3]
    combined, left, right = exchange(momentum, gradient, q_prev, owner_group, group_counts)
    return finish(combined, left, right, owner_group, group_counts, cap, share)


def solution(mesh):
    return jax.shard_map(
        shards,
        mesh=mesh,
        in_specs=(
            P(None, AXES, None),
            P(None, AXES, None),
            P("group", None, "shard", None),
            P(),
            P(),
        ),
        out_specs=(P(None, AXES, None), P(None, AXES, None), P("group", None, "shard", None)),
        check_vma=False,
    )
```

```python
import math

import jax
import jax.numpy as jnp
from jax import lax
from jax.experimental import pallas as pl
from jax.experimental.pallas import tpu as pltpu
from jax.sharding import PartitionSpec as P

D = 7168
RANK = 128

stability_offset = 1e-06
momentum_decay = 0.6
AXES = ("group", "shard")
LANES = 128
VMEM_BYTES = 67_043_328
F32, BF16 = jnp.float32, jnp.bfloat16


def vmem_bytes(ref):
    rows = -(-ref.shape[-2] // 8) * 8 if ref.shape[-2] > 1 else 1
    lanes = -(-ref.shape[-1] // LANES) * LANES
    return math.prod(ref.shape[:-2]) * rows * lanes * jnp.dtype(ref.dtype).itemsize


def scalar_slot(owner_ref, e, experts, cap):
    own = owner_ref[e]
    slot = jnp.int32(0)
    for other in range(experts):
        hit = (owner_ref[other] == own) & (other < e)
        slot = slot + jnp.where(hit, 1, 0)
    return own, slot, jnp.minimum(slot, cap - 1)


def exchange(momentum, gradient, q_prev, owner_group, group_counts):
    experts, block, hidden = momentum.shape
    cap, share, rank = q_prev.shape[1:]
    groups, nz = lax.axis_size("group"), lax.axis_size("shard")
    m = groups // 2
    a = 2 ** ((m.bit_length() - 1) // 2)
    b = m // a
    rb = share // groups
    hb = hidden // LANES
    L = hb // m
    L2 = L // 2
    half = rank // 2
    subs = nz // L
    nr = half // subs
    q_view = q_prev.reshape(cap, 2, m, rb, rank)

    counts = [
        ("qcore", 1), ("qplane", m - 1), ("qz", nz - 1), ("qxy", a + b - 2),
        ("qdiag", 2 * (a - 1) * (b - 1)), ("qback", 1),
        ("ncore", 1), ("n1", a + b - 2), ("n2", a + b - 2), ("nz", nz - 1),
        ("rcore", 1), ("p1", a + b - 2), ("p2", a + b - 2), ("rz", nz - 1),
        ("gz", nz - 1), ("gxy", a + b - 2), ("gdiag", 2 * (a - 1) * (b - 1)), ("gback", 1),
    ]
    base, total = {}, 0
    for name, n in counts:
        base[name] = total
        total += n

    def kernel(
        mom, grad, q_in, owner_in, counts_in,
        comb, left, right_out,
        mom_buf, grad_buf, q_own, qp, qc_land, qc, qp_land, Q,
        left_raw, n_own, nc_land, n_chip, n1_land, n_a, n_b, n2_land, n_place, nz_land, weights,
        pt, c_land, cs, p1a, p1b, s2a, s2b, p2a, p2b, ps, z_land, R,
        send, recv, load_sem, owner_ref, counts_ref, small_sem,
    ):
        g, s = lax.axis_index("group"), lax.axis_index("shard")
        c = lax.rem(g, 2)
        p = g // 2
        y, x = p // b, lax.rem(p, b)
        oc = 1 - c

        def up(v, k, n):
            return lax.rem(v + k, n)

        def down(v, k, n):
            return lax.rem(v + n - k, n)

        def copy(name, e, k, src, dst, device):
            return pltpu.make_async_remote_copy(
                src_ref=src, dst_ref=dst,
                send_sem=send.at[e, base[name] + k], recv_sem=recv.at[e, base[name] + k],
                device_id=device, device_id_type=pl.DeviceIdType.MESH,
            )

        def dev(yy, xx):
            return ((yy * b + xx) * 2 + c, s)

        core = (p * 2 + oc, s)

        def family(name, e):
            out = []
            if name == "qcore":
                out.append((qp.at[e, oc], qc_land.at[e], qc_land.at[e], core))
            elif name == "qplane":
                for k in range(1, m):
                    to = up(p, k, m)
                    out.append((qc.at[e, to], qp_land.at[e, k - 1], qp_land.at[e, k - 1], (to * 2 + c, s)))
            elif name == "qz":
                for k in range(1, nz):
                    here = Q.at[e, c, p, s]
                    out.append((here, here, Q.at[e, c, p, down(s, k, nz)], (g, up(s, k, nz))))
            elif name == "gz":
                def piece(at):
                    rows = pl.ds(pl.multiple_of((at // L) * nr, nr), nr)
                    return R.at[e, c, p * L + lax.rem(at, L), rows]
                for k in range(1, nz):
                    out.append((piece(s), piece(s), piece(down(s, k, nz)), (g, up(s, k, nz))))
            elif name in ("qxy", "gxy"):
                whole = q_place if name == "qxy" else r_place
                for k in range(1, a):
                    out.append((whole(e, y, x), whole(e, y, x), whole(e, down(y, k, a), x), dev(up(y, k, a), x)))
                for k in range(1, b):
                    out.append((whole(e, y, x), whole(e, y, x), whole(e, y, down(x, k, b)), dev(y, up(x, k, b))))
            elif name in ("qdiag", "gdiag"):
                part = q_half if name == "qdiag" else r_half
                for k in range(1, a):
                    for j in range(1, b):
                        xx = down(x, j, b)
                        out.append((part(e, y, xx, 0), part(e, y, xx, 0), part(e, down(y, k, a), xx, 0), dev(up(y, k, a), x)))
                for k in range(1, a):
                    for j in range(1, b):
                        yy = down(y, k, a)
                        out.append((part(e, yy, x, 1), part(e, yy, x, 1), part(e, yy, down(x, j, b), 1), dev(y, up(x, j, b))))
            elif name == "qback":
                out.append((Q.at[e, c], Q.at[e, c], Q.at[e, oc], core))
            elif name == "gback":
                out.append((R.at[e, c], R.at[e, c], R.at[e, oc], core))
            elif name == "ncore":
                out.append((n_own.at[e], nc_land.at[e], nc_land.at[e], core))
            elif name == "n1":
                for k in range(1, a):
                    out.append((n_chip.at[e], n1_land.at[e, k - 1], n1_land.at[e, k - 1], dev(up(y, k, a), x)))
                for k in range(1, b):
                    at = n1_land.at[e, a - 1 + k - 1]
                    out.append((n_chip.at[e], at, at, dev(y, up(x, k, b))))
            elif name == "n2":
                for k in range(1, b):
                    out.append((n_a.at[e], n2_land.at[e, k - 1], n2_land.at[e, k - 1], dev(y, up(x, k, b))))
                for k in range(1, a):
                    at = n2_land.at[e, b - 1 + k - 1]
                    out.append((n_b.at[e], at, at, dev(up(y, k, a), x)))
            elif name == "nz":
                for k in range(1, nz):
                    out.append((n_place.at[e], nz_land.at[e, k - 1], nz_land.at[e, k - 1], (g, up(s, k, nz))))
            elif name == "rcore":
                out.append((pt.at[e, oc], c_land.at[e], c_land.at[e], core))
            elif name == "p1":
                for k in range(1, a):
                    out.append((cs.at[e, 0, up(y, k, a)], p1a.at[e, k - 1], p1a.at[e, k - 1], dev(up(y, k, a), x)))
                for k in range(1, b):
                    out.append((cs.at[e, 1, :, up(x, k, b)], p1b.at[e, k - 1], p1b.at[e, k - 1], dev(y, up(x, k, b))))
            elif name == "p2":
                for k in range(1, b):
                    out.append((s2a.at[e, up(x, k, b)], p2a.at[e, k - 1], p2a.at[e, k - 1], dev(y, up(x, k, b))))
                for k in range(1, a):
                    out.append((s2b.at[e, up(y, k, a)], p2b.at[e, k - 1], p2b.at[e, k - 1], dev(up(y, k, a), x)))
            elif name == "rz":
                for k in range(1, nz):
                    at = up(s, k, nz)
                    rows = pl.ds(pl.multiple_of((at // L) * nr, nr), nr)
                    out.append((ps.at[e, lax.rem(at, L), rows], z_land.at[e, k - 1], z_land.at[e, k - 1], (g, at)))
            return out

        def q_place(e, yy, xx):
            return Q.at[e, c, yy * b + xx]

        def q_half(e, yy, xx, h):
            return Q.at[e, c, yy * b + xx, pl.ds(h * (nz // 2), nz // 2)]

        def r_place(e, yy, xx):
            return R.at[e, c, pl.ds((yy * b + xx) * L, L)]

        def r_half(e, yy, xx, h):
            return R.at[e, c, pl.ds((yy * b + xx) * L + h * L2, L2)]

        def start(name, e):
            for k, (src, dst, _, device) in enumerate(family(name, e)):
                copy(name, e, k, src, dst, device).start()

        def arrived(name, e):
            for k, (src, _, dst, device) in enumerate(family(name, e)):
                copy(name, e, k, src, dst, device).wait_recv()

        def sent(name, e):
            for k, (src, dst, _, device) in enumerate(family(name, e)):
                copy(name, e, k, src, dst, device).wait_send()

        def loads(e):
            at = lax.rem(e, 2)
            return (
                pltpu.make_async_copy(mom.at[e], mom_buf.at[at], load_sem.at[at, 0]),
                pltpu.make_async_copy(grad.at[e], grad_buf.at[at], load_sem.at[at, 1]),
            )

        small = [
            pltpu.make_async_copy(q_in, q_own, small_sem.at[0]),
            pltpu.make_async_copy(owner_in, owner_ref, small_sem.at[1]),
            pltpu.make_async_copy(counts_in, counts_ref, small_sem.at[2]),
        ]
        for one in small:
            one.start()
        for e in range(min(2, experts)):
            for one in loads(e):
                one.start()

        barrier = pltpu.get_barrier_semaphore()
        for k in range(1, groups):
            pl.semaphore_signal(barrier, inc=1, device_id=(up(g, k, groups), s), device_id_type=pl.DeviceIdType.MESH)
        for k in range(1, nz):
            pl.semaphore_signal(barrier, inc=1, device_id=(g, up(s, k, nz)), device_id_type=pl.DeviceIdType.MESH)

        for one in small:
            one.wait()

        @pl.loop(0, experts)
        def _(e):
            own, slot, at = scalar_slot(owner_ref, e, experts, cap)
            live = (slot < counts_ref[own]) & (own == g)
            factor = jnp.where(live, 1.0, 0.0).astype(F32)
            for h in range(2):
                qp[e, h] = (q_own[at, h].astype(F32) * factor).astype(BF16)

        pl.semaphore_wait(barrier, groups + nz - 2)

        @pl.loop(0, experts)
        def _(e):
            start("qcore", e)

        def stage_q0(e):
            arrived("qcore", e)
            qc[e] = qp[e, c] + qc_land[e]
            start("qplane", e)

        def stage_q1(e):
            arrived("qplane", e)
            mine = qc[e, p]
            for k in range(m - 1):
                mine = mine + qp_land[e, k]
            Q[e, c, p, s] = mine
            start("qz", e)

        def stage_combine(e):
            for one in loads(e):
                one.wait()
            at = lax.rem(e, 2)
            comb[e] = (mom_buf[at].astype(F32) + grad_buf[at].astype(F32)).astype(BF16)

            @pl.when(e + 2 < experts)
            def _():
                for one in loads(e + 2):
                    one.start()

        def relay(before, after):
            def stage(e):
                arrived(before, e)
                start(after, e)
            return stage

        def merge(parts):
            tot = parts[0]
            for one in parts[1:]:
                tot = tot + one
            scale = lax.rsqrt(tot + stability_offset)
            finite = tot < jnp.inf
            rows = [jnp.where(finite, jnp.sqrt(one + stability_offset) * scale, 0.0) for one in parts]
            rows += [jnp.zeros_like(tot)] * (8 - len(rows))
            weights[...] = jnp.concatenate(rows, axis=0).T
            mine = weights[pl.ds(pl.multiple_of(c * half, half), half), :]
            return tot, [mine[:, k:k + 1] for k in range(len(parts))]

        def stage_left(e):
            arrived("qback", e)
            acc = jnp.zeros((block, rank), F32)
            span = share // 2
            for z in range(nz):
                for h in range(2):
                    rows = Q[e, h, :, z].reshape(span, rank)
                    lo = z * share + h * span
                    acc = acc + jnp.dot(comb[e, :, lo:lo + span], rows, preferred_element_type=F32)
            left_raw[e] = acc
            squares = jnp.sum(acc * acc, axis=0, keepdims=True)
            n_own[e] = squares
            start("ncore", e)
            unit_t = (acc * lax.rsqrt(squares + stability_offset)).T.astype(BF16)
            wide = 2 * LANES
            for j in range(hidden // wide):
                res = jnp.dot(unit_t, comb[e, :, j * wide:(j + 1) * wide], preferred_element_type=F32).astype(BF16)
                for i in range(2):
                    for h in range(2):
                        pt[e, h, 2 * j + i] = res[h * half:(h + 1) * half, i * LANES:(i + 1) * LANES]
            start("rcore", e)

        def stage_chip(e):
            arrived("ncore", e)
            tot, (w_own, w_land) = merge([n_own[e], nc_land[e]])
            n_chip[e] = tot
            start("n1", e)
            arrived("rcore", e)
            for h in range(2):
                for i in range(L2):
                    for pp in range(m):
                        at = pp * L + h * L2 + i
                        cs[e, h, pp // b, pp % b, i] = (
                            pt[e, c, at].astype(F32) * w_own + c_land[e, at].astype(F32) * w_land
                        ).astype(BF16)
            start("p1", e)

        def stage_p1(e):
            arrived("n1", e)
            tot_a, w_a = merge([n_chip[e]] + [n1_land[e, k] for k in range(a - 1)])
            tot_b, w_b = merge([n_chip[e]] + [n1_land[e, a - 1 + k] for k in range(b - 1)])
            n_a[e] = tot_a
            n_b[e] = tot_b
            start("n2", e)
            arrived("p1", e)
            for i in range(b):
                tot = cs[e, 0, y, i].astype(F32) * w_a[0]
                for k in range(a - 1):
                    tot = tot + p1a[e, k, i].astype(F32) * w_a[k + 1]
                s2a[e, i] = tot.astype(BF16)
            for i in range(a):
                tot = cs[e, 1, i, x].astype(F32) * w_b[0]
                for k in range(b - 1):
                    tot = tot + p1b[e, k, i].astype(F32) * w_b[k + 1]
                s2b[e, i] = tot.astype(BF16)
            start("p2", e)

        def stage_p2(e):
            arrived("n2", e)
            tot_a, w_a = merge([n_a[e]] + [n2_land[e, k] for k in range(b - 1)])
            _, w_b = merge([n_b[e]] + [n2_land[e, b - 1 + k] for k in range(a - 1)])
            n_place[e] = tot_a
            start("nz", e)
            arrived("p2", e)
            tot = s2a[e, x].astype(F32) * w_a[0]
            for k in range(b - 1):
                tot = tot + p2a[e, k].astype(F32) * w_a[k + 1]
            ps[e, 0:L2] = tot.astype(BF16)
            tot = s2b[e, y].astype(F32) * w_b[0]
            for k in range(a - 1):
                tot = tot + p2b[e, k].astype(F32) * w_b[k + 1]
            ps[e, L2:L] = tot.astype(BF16)
            start("rz", e)

        def stage_rz(e):
            arrived("nz", e)
            at = pl.multiple_of((s // L) * nr, nr)
            total_squares, w = merge([n_place[e]] + [nz_land[e, k] for k in range(nz - 1)])
            sub = pl.ds(pl.multiple_of(c * half + at, nr), nr)
            w = [weights[sub, k:k + 1] for k in range(nz)]
            arrived("rz", e)
            rows = pl.ds(at, nr)
            tot = ps[e, lax.rem(s, L), rows].astype(F32) * w[0]
            for k in range(nz - 1):
                tot = tot + z_land[e, k].astype(F32) * w[k + 1]
            R[e, c, p * L + lax.rem(s, L), rows] = tot.astype(BF16)
            start("gz", e)
            left[e] = (left_raw[e] * lax.rsqrt(total_squares + stability_offset)).astype(BF16)

        def stage_done(e):
            arrived("gback", e)
            for h in range(2):
                right_out[e, h] = R[e, h]
            for name, _ in counts:
                sent(name, e)

        stages = [
            (0, stage_q0),
            (2, stage_q1),
            (4, relay("qz", "qxy")),
            (6, relay("qxy", "qdiag")),
            (8, relay("qdiag", "qback")),
            (0, stage_combine),
            (9, stage_left),
            (10, stage_chip),
            (11, stage_p1),
            (12, stage_p2),
            (14, stage_rz),
            (16, relay("gz", "gxy")),
            (17, relay("gxy", "gdiag")),
            (18, relay("gdiag", "gback")),
            (19, stage_done),
        ]

        @pl.loop(0, experts + 19)
        def _(t):
            for offset, stage in stages:
                @pl.when((t >= offset) & (t < offset + experts))
                def _():
                    stage(t - offset)

    E = experts
    scratch = [
        pltpu.VMEM((2, block, hidden), BF16),
        pltpu.VMEM((2, block, hidden), BF16),
        pltpu.VMEM((cap, 2, m, rb, rank), BF16),
        pltpu.VMEM((E, 2, m, rb, rank), BF16),
        pltpu.VMEM((E, m, rb, rank), BF16),
        pltpu.VMEM((E, m, rb, rank), BF16),
        pltpu.VMEM((E, m - 1, rb, rank), BF16),
        pltpu.VMEM((E, 2, m, nz, rb, rank), BF16),
        pltpu.VMEM((E, block, rank), F32),
        pltpu.VMEM((E, 1, rank), F32),
        pltpu.VMEM((E, 1, rank), F32),
        pltpu.VMEM((E, 1, rank), F32),
        pltpu.VMEM((E, a + b - 2, 1, rank), F32),
        pltpu.VMEM((E, 1, rank), F32),
        pltpu.VMEM((E, 1, rank), F32),
        pltpu.VMEM((E, a + b - 2, 1, rank), F32),
        pltpu.VMEM((E, 1, rank), F32),
        pltpu.VMEM((E, nz - 1, 1, rank), F32),
        pltpu.VMEM((rank, 8), F32),
        pltpu.VMEM((E, 2, hb, half, LANES), BF16),
        pltpu.VMEM((E, hb, half, LANES), BF16),
        pltpu.VMEM((E, 2, a, b, L2, half, LANES), BF16),
        pltpu.VMEM((E, a - 1, b, L2, half, LANES), BF16),
        pltpu.VMEM((E, b - 1, a, L2, half, LANES), BF16),
        pltpu.VMEM((E, b, L2, half, LANES), BF16),
        pltpu.VMEM((E, a, L2, half, LANES), BF16),
        pltpu.VMEM((E, b - 1, L2, half, LANES), BF16),
        pltpu.VMEM((E, a - 1, L2, half, LANES), BF16),
        pltpu.VMEM((E, L, half, LANES), BF16),
        pltpu.VMEM((E, nz - 1, nr, LANES), BF16),
        pltpu.VMEM((E, 2, hb, half, LANES), BF16),
    ]
    outputs = 2 * E * (block * (hidden + rank) + hidden * rank)
    limit = min(VMEM_BYTES, sum(map(vmem_bytes, scratch)) + outputs + 1_500_000)
    hbm = pl.BlockSpec(memory_space=pltpu.HBM)
    return pl.pallas_call(
        kernel,
        name="exchange",
        out_shape=(
            jax.ShapeDtypeStruct((E, block, hidden), BF16),
            jax.ShapeDtypeStruct((E, block, rank), BF16),
            jax.ShapeDtypeStruct((E, 2, hb, half, LANES), BF16),
        ),
        in_specs=[hbm] * 5,
        out_specs=(pl.BlockSpec(memory_space=pltpu.VMEM),) * 3,
        scratch_shapes=scratch + [
            pltpu.SemaphoreType.DMA((E, total)),
            pltpu.SemaphoreType.DMA((E, total)),
            pltpu.SemaphoreType.DMA((2, 2)),
            pltpu.SMEM((E,), jnp.int32),
            pltpu.SMEM((groups,), jnp.int32),
            pltpu.SemaphoreType.DMA((3,)),
        ],
        compiler_params=pltpu.CompilerParams(
            collective_id=0, has_side_effects=True, vmem_limit_bytes=limit
        ),
    )(momentum, gradient, q_view, owner_group, group_counts)


def finish(combined, left, right, owner_group, group_counts, cap, share):
    experts, block, hidden = combined.shape
    rank = left.shape[2]
    hb, half = right.shape[2:4]
    own_blocks = share // LANES

    def kernel(
        owner_in, counts_in, comb, left_ref, right_ref, mom_out, upd_out, q_out,
        kept, owner_ref, counts_ref, small_sem,
    ):
        e = pl.program_id(0)
        small = (
            pltpu.make_async_copy(owner_in, owner_ref, small_sem.at[0]),
            pltpu.make_async_copy(counts_in, counts_ref, small_sem.at[1]),
        )

        @pl.when(e == 0)
        def _():
            for one in small:
                one.start()

        me, s = lax.axis_index("group"), lax.axis_index("shard")

        def block_of(i):
            return jnp.concatenate([right_ref[e, 0, i], right_ref[e, 1, i]], axis=0).astype(F32)

        squares = jnp.zeros((rank, LANES), F32)
        for i in range(hb):
            one = block_of(i)
            squares = squares + one * one
        scale = lax.rsqrt(jnp.sum(squares, axis=1, keepdims=True) / hidden + stability_offset)

        unit = left_ref[e]
        for j in range(hb // 2):
            raw = jnp.concatenate([block_of(2 * j), block_of(2 * j + 1)], axis=1)
            span = slice(2 * j * LANES, (2 * j + 2) * LANES)
            low = jnp.dot(unit, raw.astype(BF16), preferred_element_type=F32)
            mom_out[0, :, span] = (
                comb[e, :, span].astype(F32) - (1.0 - momentum_decay) * low
            ).astype(BF16)
            new = (raw * scale).astype(BF16)
            upd_out[0, :, span] = (
                jnp.dot(unit, new, preferred_element_type=F32) * math.sqrt(D / RANK)
            ).astype(BF16)

        @pl.when(e == 0)
        def _():
            kept[...] = jnp.zeros_like(kept)
            for one in small:
                one.wait()

        own, slot, at = scalar_slot(owner_ref, e, experts, cap)

        @pl.when((slot < counts_ref[own]) & (own == me))
        def _():
            for i in range(own_blocks):
                kept[at, i] = (block_of(s * own_blocks + i) * scale).astype(BF16).astype(F32)

        @pl.when(e == experts - 1)
        def _():
            for j in range(cap):
                for i in range(own_blocks):
                    q_out[0, j, i * LANES:(i + 1) * LANES, :] = kept[j, i].T.astype(BF16)

    hbm = pl.BlockSpec(memory_space=pltpu.HBM)
    vmem = pl.BlockSpec(memory_space=pltpu.VMEM)
    row = pl.BlockSpec((1, block, hidden), lambda e: (e, 0, 0))
    return pl.pallas_call(
        kernel,
        name="finish",
        grid=(experts,),
        out_shape=(
            jax.ShapeDtypeStruct(combined.shape, BF16),
            jax.ShapeDtypeStruct(combined.shape, BF16),
            jax.ShapeDtypeStruct((1, cap, share, rank), BF16),
        ),
        in_specs=[
            hbm, hbm, vmem, vmem, vmem,
        ],
        out_specs=(row, row, pl.BlockSpec((1, cap, share, rank), lambda e: (0, 0, 0, 0))),
        scratch_shapes=[
            pltpu.VMEM((cap, own_blocks, rank, LANES), F32),
            pltpu.SMEM(owner_group.shape, jnp.int32),
            pltpu.SMEM(group_counts.shape, jnp.int32),
            pltpu.SemaphoreType.DMA((2,)),
        ],
        compiler_params=pltpu.CompilerParams(
            dimension_semantics=("arbitrary",), vmem_limit_bytes=24_000_000
        ),
    )(owner_group, group_counts, combined, left, right)


def shards(momentum, gradient, q_prev, owner_group, group_counts):
    cap, share = q_prev.shape[1:3]
    combined, left, right = exchange(momentum, gradient, q_prev, owner_group, group_counts)
    return finish(combined, left, right, owner_group, group_counts, cap, share)


def solution(mesh):
    return jax.shard_map(
        shards,
        mesh=mesh,
        in_specs=(
            P(None, AXES, None),
            P(None, AXES, None),
            P("group", None, "shard", None),
            P(),
            P(),
        ),
        out_specs=(P(None, AXES, None), P(None, AXES, None), P("group", None, "shard", None)),
        check_vma=False,
    )
```

```python
import math

import jax
import jax.numpy as jnp
from jax import lax
from jax.experimental import pallas as pl
from jax.experimental.pallas import tpu as pltpu
from jax.sharding import PartitionSpec as P

D = 7168
RANK = 128

stability_offset = 1e-06
momentum_decay = 0.6
AXES = ("group", "shard")
LANES = 128
VMEM_BYTES = 67_043_328
F32, BF16 = jnp.float32, jnp.bfloat16


def vmem_bytes(ref):
    rows = -(-ref.shape[-2] // 8) * 8 if ref.shape[-2] > 1 else 1
    lanes = -(-ref.shape[-1] // LANES) * LANES
    return math.prod(ref.shape[:-2]) * rows * lanes * jnp.dtype(ref.dtype).itemsize


def scalar_slot(owner_ref, e, experts, cap):
    own = owner_ref[e]
    slot = jnp.int32(0)
    for other in range(experts):
        hit = (owner_ref[other] == own) & (other < e)
        slot = slot + jnp.where(hit, 1, 0)
    return own, slot, jnp.minimum(slot, cap - 1)


def exchange(momentum, gradient, q_prev, plan):
    experts, block, hidden = momentum.shape
    cap, share, rank = q_prev.shape[1:]
    groups, nz = lax.axis_size("group"), lax.axis_size("shard")
    m = groups // 2
    a = 2 ** ((m.bit_length() - 1) // 2)
    b = m // a
    rb = share // groups
    hb = hidden // LANES
    own_blocks = share // LANES
    L = hb // m
    L2 = L // 2
    half = rank // 2
    subs = nz // L
    nr = half // subs
    q_view = q_prev.reshape(cap, 2, m, rb, rank)
    plan_shape = plan.shape

    counts = [
        ("qz", nz - 1), ("qxy", a + b - 2),
        ("qdiag", 2 * (a - 1) * (b - 1)), ("qback", 1),
        ("ncore", 1), ("n1", a + b - 2), ("n2", a + b - 2), ("nz", nz - 1),
        ("rcore", 1), ("p1", a + b - 2), ("p2", a + b - 2), ("rz", nz - 1),
        ("gz", nz - 1), ("gxy", a + b - 2), ("gdiag", 2 * (a - 1) * (b - 1)), ("gback", 1),
    ]
    base, total = {}, 0
    for name, n in counts:
        base[name] = total
        total += n

    def kernel(
        mom, grad, q_ref, plan_in,
        comb, upd, q_out,
        mom_buf, grad_buf, slots, Q,
        left_raw, left, kept, n_own, nc_land, n_chip, n1_land, n_a, n_b, n2_land, n_place, nz_land, weights,
        pt, c_land, cs, p1a, p1b, s2a, s2b, p2a, p2b, ps, z_land, R,
        send, recv, slot_send, slot_recv, load_sem, plan, plan_sem,
    ):
        g, s = lax.axis_index("group"), lax.axis_index("shard")
        c = lax.rem(g, 2)
        p = g // 2
        y, x = p // b, lax.rem(p, b)
        oc = 1 - c

        def up(v, k, n):
            return lax.rem(v + k, n)

        def down(v, k, n):
            return lax.rem(v + n - k, n)

        def copy(name, e, k, src, dst, device):
            return pltpu.make_async_remote_copy(
                src_ref=src, dst_ref=dst,
                send_sem=send.at[e, base[name] + k], recv_sem=recv.at[e, base[name] + k],
                device_id=device, device_id_type=pl.DeviceIdType.MESH,
            )

        def dev(yy, xx):
            return ((yy * b + xx) * 2 + c, s)

        core = (p * 2 + oc, s)

        def family(name, e):
            out = []
            if name == "qz":
                for k in range(1, nz):
                    here = Q.at[e, c, p, s]
                    out.append((here, here, Q.at[e, c, p, down(s, k, nz)], (g, up(s, k, nz))))
            elif name == "gz":
                def piece(at):
                    rows = pl.ds(pl.multiple_of((at // L) * nr, nr), nr)
                    return R.at[e, c, p * L + lax.rem(at, L), rows]
                for k in range(1, nz):
                    out.append((piece(s), piece(s), piece(down(s, k, nz)), (g, up(s, k, nz))))
            elif name in ("qxy", "gxy"):
                whole = q_place if name == "qxy" else r_place
                for k in range(1, a):
                    out.append((whole(e, y, x), whole(e, y, x), whole(e, down(y, k, a), x), dev(up(y, k, a), x)))
                for k in range(1, b):
                    out.append((whole(e, y, x), whole(e, y, x), whole(e, y, down(x, k, b)), dev(y, up(x, k, b))))
            elif name in ("qdiag", "gdiag"):
                part = q_half if name == "qdiag" else r_half
                for k in range(1, a):
                    for j in range(1, b):
                        xx = down(x, j, b)
                        out.append((part(e, y, xx, 0), part(e, y, xx, 0), part(e, down(y, k, a), xx, 0), dev(up(y, k, a), x)))
                for k in range(1, a):
                    for j in range(1, b):
                        yy = down(y, k, a)
                        out.append((part(e, yy, x, 1), part(e, yy, x, 1), part(e, yy, down(x, j, b), 1), dev(y, up(x, j, b))))
            elif name == "qback":
                out.append((Q.at[e, c], Q.at[e, c], Q.at[e, oc], core))
            elif name == "gback":
                out.append((R.at[e, c], R.at[e, c], R.at[e, oc], core))
            elif name == "ncore":
                out.append((n_own.at[e], nc_land.at[e], nc_land.at[e], core))
            elif name == "n1":
                for k in range(1, a):
                    out.append((n_chip.at[e], n1_land.at[e, k - 1], n1_land.at[e, k - 1], dev(up(y, k, a), x)))
                for k in range(1, b):
                    at = n1_land.at[e, a - 1 + k - 1]
                    out.append((n_chip.at[e], at, at, dev(y, up(x, k, b))))
            elif name == "n2":
                for k in range(1, b):
                    out.append((n_a.at[e], n2_land.at[e, k - 1], n2_land.at[e, k - 1], dev(y, up(x, k, b))))
                for k in range(1, a):
                    at = n2_land.at[e, b - 1 + k - 1]
                    out.append((n_b.at[e], at, at, dev(up(y, k, a), x)))
            elif name == "nz":
                for k in range(1, nz):
                    out.append((n_place.at[e], nz_land.at[e, k - 1], nz_land.at[e, k - 1], (g, up(s, k, nz))))
            elif name == "rcore":
                out.append((pt.at[e, oc], c_land.at[e], c_land.at[e], core))
            elif name == "p1":
                for k in range(1, a):
                    out.append((cs.at[e, 0, up(y, k, a)], p1a.at[e, k - 1], p1a.at[e, k - 1], dev(up(y, k, a), x)))
                for k in range(1, b):
                    out.append((cs.at[e, 1, :, up(x, k, b)], p1b.at[e, k - 1], p1b.at[e, k - 1], dev(y, up(x, k, b))))
            elif name == "p2":
                for k in range(1, b):
                    out.append((s2a.at[e, up(x, k, b)], p2a.at[e, k - 1], p2a.at[e, k - 1], dev(y, up(x, k, b))))
                for k in range(1, a):
                    out.append((s2b.at[e, up(y, k, a)], p2b.at[e, k - 1], p2b.at[e, k - 1], dev(up(y, k, a), x)))
            elif name == "rz":
                for k in range(1, nz):
                    at = up(s, k, nz)
                    rows = pl.ds(pl.multiple_of((at // L) * nr, nr), nr)
                    out.append((ps.at[e, lax.rem(at, L), rows], z_land.at[e, k - 1], z_land.at[e, k - 1], (g, at)))
            return out

        def q_place(e, yy, xx):
            return Q.at[e, c, yy * b + xx]

        def q_half(e, yy, xx, h):
            return Q.at[e, c, yy * b + xx, pl.ds(h * (nz // 2), nz // 2)]

        def r_place(e, yy, xx):
            return R.at[e, c, pl.ds((yy * b + xx) * L, L)]

        def r_half(e, yy, xx, h):
            return R.at[e, c, pl.ds((yy * b + xx) * L + h * L2, L2)]

        def start(name, e):
            for k, (src, dst, _, device) in enumerate(family(name, e)):
                copy(name, e, k, src, dst, device).start()

        def arrived(name, e):
            for k, (src, _, dst, device) in enumerate(family(name, e)):
                copy(name, e, k, src, dst, device).wait_recv()

        def sent(name, e):
            for k, (src, dst, _, device) in enumerate(family(name, e)):
                copy(name, e, k, src, dst, device).wait_send()

        def loads(e):
            at = lax.rem(e, 2)
            return (
                pltpu.make_async_copy(mom.at[e], mom_buf.at[at], load_sem.at[at, 0]),
                pltpu.make_async_copy(grad.at[e], grad_buf.at[at], load_sem.at[at, 1]),
            )

        plan_load = pltpu.make_async_copy(plan_in, plan, plan_sem)
        plan_load.start()
        for e in range(min(2, experts)):
            for one in loads(e):
                one.start()

        barrier = pltpu.get_barrier_semaphore()
        for k in range(1, groups):
            pl.semaphore_signal(barrier, inc=1, device_id=(up(g, k, groups), s), device_id_type=pl.DeviceIdType.MESH)
        for k in range(1, nz):
            pl.semaphore_signal(barrier, inc=1, device_id=(g, up(s, k, nz)), device_id_type=pl.DeviceIdType.MESH)

        def slot_copy(k):
            to = up(g, k, groups)
            return pltpu.make_async_remote_copy(
                src_ref=q_ref.at[:, lax.rem(to, 2), to // 2], dst_ref=slots.at[g],
                send_sem=slot_send.at[k - 1], recv_sem=slot_recv.at[k - 1],
                device_id=(to, s), device_id_type=pl.DeviceIdType.MESH,
            )

        slots[g] = q_ref[:, c, p]
        kept[...] = jnp.zeros_like(kept)
        plan_load.wait()
        pl.semaphore_wait(barrier, groups + nz - 2)
        for k in range(1, groups):
            slot_copy(k).start()
        for k in range(1, groups):
            slot_copy(k).wait_recv()

        @pl.loop(0, experts)
        def _(e):
            own, slot, at = scalar_slot(plan, e, experts, cap)
            factor = jnp.where(slot < plan[experts + own], 1.0, 0.0).astype(F32)
            Q[e, c, p, s] = (slots[own, at].astype(F32) * factor).astype(BF16)
            start("qz", e)

        def stage_combine(e):
            for one in loads(e):
                one.wait()
            at = lax.rem(e, 2)
            comb[e] = (mom_buf[at].astype(F32) + grad_buf[at].astype(F32)).astype(BF16)

            @pl.when(e + 2 < experts)
            def _():
                for one in loads(e + 2):
                    one.start()

        def relay(before, after):
            def stage(e):
                arrived(before, e)
                start(after, e)
            return stage

        def merge(parts):
            tot = parts[0]
            for one in parts[1:]:
                tot = tot + one
            scale = lax.rsqrt(tot + stability_offset)
            finite = tot < jnp.inf
            rows = [jnp.where(finite, jnp.sqrt(one + stability_offset) * scale, 0.0) for one in parts]
            rows += [jnp.zeros_like(tot)] * (8 - len(rows))
            weights[...] = jnp.concatenate(rows, axis=0).T
            mine = weights[pl.ds(pl.multiple_of(c * half, half), half), :]
            return tot, [mine[:, k:k + 1] for k in range(len(parts))]

        def stage_left(e):
            arrived("qback", e)
            acc = jnp.zeros((block, rank), F32)
            span = share // 2
            for z in range(nz):
                for h in range(2):
                    rows = Q[e, h, :, z].reshape(span, rank)
                    lo = z * share + h * span
                    acc = acc + jnp.dot(comb[e, :, lo:lo + span], rows, preferred_element_type=F32)
            left_raw[e] = acc
            squares = jnp.sum(acc * acc, axis=0, keepdims=True)
            n_own[e] = squares
            start("ncore", e)
            unit_t = (acc * lax.rsqrt(squares + stability_offset)).T.astype(BF16)
            wide = 2 * LANES
            for j in range(hidden // wide):
                res = jnp.dot(unit_t, comb[e, :, j * wide:(j + 1) * wide], preferred_element_type=F32).astype(BF16)
                for i in range(2):
                    for h in range(2):
                        pt[e, h, 2 * j + i] = res[h * half:(h + 1) * half, i * LANES:(i + 1) * LANES]
            start("rcore", e)

        def stage_chip(e):
            arrived("ncore", e)
            tot, (w_own, w_land) = merge([n_own[e], nc_land[e]])
            n_chip[e] = tot
            start("n1", e)
            arrived("rcore", e)
            for h in range(2):
                for i in range(L2):
                    for pp in range(m):
                        at = pp * L + h * L2 + i
                        cs[e, h, pp // b, pp % b, i] = (
                            pt[e, c, at].astype(F32) * w_own + c_land[e, at].astype(F32) * w_land
                        ).astype(BF16)
            start("p1", e)

        def stage_p1(e):
            arrived("n1", e)
            tot_a, w_a = merge([n_chip[e]] + [n1_land[e, k] for k in range(a - 1)])
            tot_b, w_b = merge([n_chip[e]] + [n1_land[e, a - 1 + k] for k in range(b - 1)])
            n_a[e] = tot_a
            n_b[e] = tot_b
            start("n2", e)
            arrived("p1", e)
            for i in range(b):
                tot = cs[e, 0, y, i].astype(F32) * w_a[0]
                for k in range(a - 1):
                    tot = tot + p1a[e, k, i].astype(F32) * w_a[k + 1]
                s2a[e, i] = tot.astype(BF16)
            for i in range(a):
                tot = cs[e, 1, i, x].astype(F32) * w_b[0]
                for k in range(b - 1):
                    tot = tot + p1b[e, k, i].astype(F32) * w_b[k + 1]
                s2b[e, i] = tot.astype(BF16)
            start("p2", e)

        def stage_p2(e):
            arrived("n2", e)
            tot_a, w_a = merge([n_a[e]] + [n2_land[e, k] for k in range(b - 1)])
            _, w_b = merge([n_b[e]] + [n2_land[e, b - 1 + k] for k in range(a - 1)])
            n_place[e] = tot_a
            start("nz", e)
            arrived("p2", e)
            tot = s2a[e, x].astype(F32) * w_a[0]
            for k in range(b - 1):
                tot = tot + p2a[e, k].astype(F32) * w_a[k + 1]
            ps[e, 0:L2] = tot.astype(BF16)
            tot = s2b[e, y].astype(F32) * w_b[0]
            for k in range(a - 1):
                tot = tot + p2b[e, k].astype(F32) * w_b[k + 1]
            ps[e, L2:L] = tot.astype(BF16)
            start("rz", e)

        def stage_rz(e):
            arrived("nz", e)
            at = pl.multiple_of((s // L) * nr, nr)
            total_squares, w = merge([n_place[e]] + [nz_land[e, k] for k in range(nz - 1)])
            sub = pl.ds(pl.multiple_of(c * half + at, nr), nr)
            w = [weights[sub, k:k + 1] for k in range(nz)]
            arrived("rz", e)
            rows = pl.ds(at, nr)
            tot = ps[e, lax.rem(s, L), rows].astype(F32) * w[0]
            for k in range(nz - 1):
                tot = tot + z_land[e, k].astype(F32) * w[k + 1]
            R[e, c, p * L + lax.rem(s, L), rows] = tot.astype(BF16)
            start("gz", e)
            left[e] = (left_raw[e] * lax.rsqrt(total_squares + stability_offset)).astype(BF16)

        def stage_done(e):
            arrived("gback", e)

            def block_of(i):
                return jnp.concatenate([R[e, 0, i], R[e, 1, i]], axis=0).astype(F32)

            squares = jnp.zeros((rank, LANES), F32)
            for i in range(hb):
                one = block_of(i)
                squares = squares + one * one
            scale = lax.rsqrt(jnp.sum(squares, axis=1, keepdims=True) / hidden + stability_offset)

            unit = left[e]
            for j in range(hb // 2):
                raw = jnp.concatenate([block_of(2 * j), block_of(2 * j + 1)], axis=1)
                span = slice(2 * j * LANES, (2 * j + 2) * LANES)
                low = jnp.dot(unit, raw.astype(BF16), preferred_element_type=F32)
                comb[e, :, span] = (
                    comb[e, :, span].astype(F32) - (1.0 - momentum_decay) * low
                ).astype(BF16)
                new = (raw * scale).astype(BF16)
                upd[e, :, span] = (
                    jnp.dot(unit, new, preferred_element_type=F32) * math.sqrt(D / RANK)
                ).astype(BF16)

            own, slot, _ = scalar_slot(plan, e, experts, cap)
            mine = (slot < plan[experts + own]) & (own == g)
            for i in range(own_blocks):
                new = (block_of(s * own_blocks + i) * scale).astype(BF16).astype(F32)
                for j in range(cap):
                    kept[j, i] += new * jnp.where(mine & (slot == j), 1.0, 0.0).astype(F32)

            for name, _ in counts:
                sent(name, e)

        stages = [
            (0, relay("qz", "qxy")),
            (2, relay("qxy", "qdiag")),
            (4, relay("qdiag", "qback")),
            (0, stage_combine),
            (5, stage_left),
            (6, stage_chip),
            (8, stage_p1),
            (10, stage_p2),
            (12, stage_rz),
            (14, relay("gz", "gxy")),
            (16, relay("gxy", "gdiag")),
            (18, relay("gdiag", "gback")),
            (19, stage_done),
        ]

        @pl.loop(0, experts + stages[-1][0])
        def _(t):
            for offset, stage in stages:
                @pl.when((t >= offset) & (t < offset + experts))
                def _():
                    stage(t - offset)

        for j in range(cap):
            for i in range(own_blocks):
                q_out[0, j, i * LANES:(i + 1) * LANES, :] = kept[j, i].T.astype(BF16)
        for k in range(1, groups):
            slot_copy(k).wait_send()

    E = experts
    scratch = [
        pltpu.VMEM((2, block, hidden), BF16),
        pltpu.VMEM((2, block, hidden), BF16),
        pltpu.VMEM((groups, cap, rb, rank), BF16),
        pltpu.VMEM((E, 2, m, nz, rb, rank), BF16),
        pltpu.VMEM((E, block, rank), F32),
        pltpu.VMEM((E, block, rank), BF16),
        pltpu.VMEM((cap, own_blocks, rank, LANES), F32),
        pltpu.VMEM((E, 1, rank), F32),
        pltpu.VMEM((E, 1, rank), F32),
        pltpu.VMEM((E, 1, rank), F32),
        pltpu.VMEM((E, a + b - 2, 1, rank), F32),
        pltpu.VMEM((E, 1, rank), F32),
        pltpu.VMEM((E, 1, rank), F32),
        pltpu.VMEM((E, a + b - 2, 1, rank), F32),
        pltpu.VMEM((E, 1, rank), F32),
        pltpu.VMEM((E, nz - 1, 1, rank), F32),
        pltpu.VMEM((rank, 8), F32),
        pltpu.VMEM((E, 2, hb, half, LANES), BF16),
        pltpu.VMEM((E, hb, half, LANES), BF16),
        pltpu.VMEM((E, 2, a, b, L2, half, LANES), BF16),
        pltpu.VMEM((E, a - 1, b, L2, half, LANES), BF16),
        pltpu.VMEM((E, b - 1, a, L2, half, LANES), BF16),
        pltpu.VMEM((E, b, L2, half, LANES), BF16),
        pltpu.VMEM((E, a, L2, half, LANES), BF16),
        pltpu.VMEM((E, b - 1, L2, half, LANES), BF16),
        pltpu.VMEM((E, a - 1, L2, half, LANES), BF16),
        pltpu.VMEM((E, L, half, LANES), BF16),
        pltpu.VMEM((E, nz - 1, nr, LANES), BF16),
        pltpu.VMEM((E, 2, hb, half, LANES), BF16),
    ]
    outputs = 2 * (2 * E * block * hidden + cap * share * rank)
    limit = min(VMEM_BYTES - outputs, sum(map(vmem_bytes, scratch)) + 11_000_000)
    hbm = pl.BlockSpec(memory_space=pltpu.HBM)
    return pl.pallas_call(
        kernel,
        name="exchange",
        out_shape=(
            jax.ShapeDtypeStruct((E, block, hidden), BF16),
            jax.ShapeDtypeStruct((E, block, hidden), BF16),
            jax.ShapeDtypeStruct((1, cap, share, rank), BF16),
        ),
        in_specs=[hbm, hbm, pl.BlockSpec(memory_space=pltpu.VMEM), hbm],
        out_specs=(pl.BlockSpec(memory_space=pltpu.VMEM),) * 3,
        scratch_shapes=scratch + [
            pltpu.SemaphoreType.DMA((E, total)),
            pltpu.SemaphoreType.DMA((E, total)),
            pltpu.SemaphoreType.DMA((groups - 1,)),
            pltpu.SemaphoreType.DMA((groups - 1,)),
            pltpu.SemaphoreType.DMA((2, 2)),
            pltpu.SMEM(plan_shape, jnp.int32),
            pltpu.SemaphoreType.DMA,
        ],
        compiler_params=pltpu.CompilerParams(
            collective_id=0, has_side_effects=True, vmem_limit_bytes=limit
        ),
    )(momentum, gradient, q_view, plan)


def store(*results):
    pieces = [one.shape[0] for one in results]

    def kernel(*refs):
        n = len(results)
        copies = []
        for at, count in enumerate(pieces):
            for e in range(count):
                copies.append((refs[at].at[e], refs[n + at].at[e]))
        sems = refs[2 * n]
        copies = [pltpu.make_async_copy(a, b, sems.at[k]) for k, (a, b) in enumerate(copies)]
        for one in copies:
            one.start()
        for one in copies:
            one.wait()

    return pl.pallas_call(
        kernel,
        name="store",
        out_shape=tuple(jax.ShapeDtypeStruct(one.shape, one.dtype) for one in results),
        in_specs=[pl.BlockSpec(memory_space=pltpu.VMEM)] * len(results),
        out_specs=(pl.BlockSpec(memory_space=pltpu.HBM),) * len(results),
        scratch_shapes=[pltpu.SemaphoreType.DMA((sum(pieces),))],
        compiler_params=pltpu.CompilerParams(vmem_limit_bytes=24_000_000),
    )(*results)


def shards(momentum, gradient, q_prev, owner_group, group_counts):
    plan = jnp.concatenate([owner_group, group_counts])
    return store(*exchange(momentum, gradient, q_prev, plan))


def solution(mesh):
    return jax.shard_map(
        shards,
        mesh=mesh,
        in_specs=(
            P(None, AXES, None),
            P(None, AXES, None),
            P("group", None, "shard", None),
            P(),
            P(),
        ),
        out_specs=(P(None, AXES, None), P(None, AXES, None), P("group", None, "shard", None)),
        check_vma=False,
    )
```

```python
import math

import jax
import jax.numpy as jnp
from jax import lax
from jax.experimental import pallas as pl
from jax.experimental.pallas import tpu as pltpu
from jax.sharding import PartitionSpec as P

D = 7168
RANK = 128

stability_offset = 1e-06
momentum_decay = 0.6
AXES = ("group", "shard")
LANES = 128
VMEM_BYTES = 67_043_328
F32, BF16 = jnp.float32, jnp.bfloat16


def vmem_bytes(ref):
    rows = -(-ref.shape[-2] // 8) * 8 if ref.shape[-2] > 1 else 1
    lanes = -(-ref.shape[-1] // LANES) * LANES
    return math.prod(ref.shape[:-2]) * rows * lanes * jnp.dtype(ref.dtype).itemsize


def scalar_slot(owner_ref, e, experts, cap):
    own = owner_ref[e]
    slot = jnp.int32(0)
    for other in range(experts):
        hit = (owner_ref[other] == own) & (other < e)
        slot = slot + jnp.where(hit, 1, 0)
    return own, slot, jnp.minimum(slot, cap - 1)


def exchange(momentum, gradient, q_prev, plan):
    experts, block, hidden = momentum.shape
    cap, share, rank = q_prev.shape[1:]
    groups, nz = lax.axis_size("group"), lax.axis_size("shard")
    m = groups // 2
    a = 2 ** ((m.bit_length() - 1) // 2)
    b = m // a
    rb = share // groups
    hb = hidden // LANES
    own_blocks = share // LANES
    L = hb // m
    L2 = L // 2
    half = rank // 2
    subs = nz // L
    nr = half // subs
    plain = experts - 3 * experts // 8
    q_view = q_prev.reshape(cap, 2, m, rb, rank)
    plan_shape = plan.shape

    counts = [
        ("fxy", a + b - 2), ("fdiag", 2 * (a - 1) * (b - 1)), ("fz", nz - 1),
        ("qz", nz - 1), ("qxy", a + b - 2),
        ("qdiag", 2 * (a - 1) * (b - 1)), ("qback", 1),
        ("ncore", 1), ("n1", a + b - 2), ("n2", a + b - 2), ("nz", nz - 1),
        ("rcore", 1), ("p1", a + b - 2), ("p2", a + b - 2), ("rz", nz - 1),
        ("gz", nz - 1), ("gxy", a + b - 2), ("gdiag", 2 * (a - 1) * (b - 1)), ("gback", 1),
    ]
    base, total = {}, 0
    for name, n in counts:
        base[name] = total
        total += n

    def kernel(
        mom, grad, q_ref, plan_in,
        comb, upd, q_out,
        mom_buf, grad_buf, slots, Q,
        left_raw, left, kept, n_own, nc_land, n_chip, n1_land, n_a, n_b, n2_land, n_place, nz_land, weights,
        pt, c_land, cs, p1a, p1b, s2a, s2b, p2a, p2b, ps, z_land, R,
        send, recv, slot_send, slot_recv, load_sem, plan, plan_sem,
    ):
        g, s = lax.axis_index("group"), lax.axis_index("shard")
        c = lax.rem(g, 2)
        p = g // 2
        y, x = p // b, lax.rem(p, b)
        oc = 1 - c

        def up(v, k, n):
            return lax.rem(v + k, n)

        def down(v, k, n):
            return lax.rem(v + n - k, n)

        def copy(name, e, k, src, dst, device):
            return pltpu.make_async_remote_copy(
                src_ref=src, dst_ref=dst,
                send_sem=send.at[e, base[name] + k], recv_sem=recv.at[e, base[name] + k],
                device_id=device, device_id_type=pl.DeviceIdType.MESH,
            )

        def dev(yy, xx):
            return ((yy * b + xx) * 2 + c, s)

        core = (p * 2 + oc, s)

        def family(name, e):
            out = []
            if name == "fxy":
                here = f_place(e, y, x)
                for k in range(1, a):
                    out.append((here, here, f_place(e, down(y, k, a), x), dev(up(y, k, a), x)))
                for k in range(1, b):
                    out.append((here, here, f_place(e, y, down(x, k, b)), dev(y, up(x, k, b))))
            elif name == "fz":
                for k in range(1, nz):
                    here = Q.at[e, c, :, s]
                    out.append((here, here, Q.at[e, c, :, down(s, k, nz)], (g, up(s, k, nz))))
            elif name == "qz":
                for k in range(1, nz):
                    here = Q.at[e, c, p, s]
                    out.append((here, here, Q.at[e, c, p, down(s, k, nz)], (g, up(s, k, nz))))
            elif name == "gz":
                def piece(at):
                    rows = pl.ds(pl.multiple_of((at // L) * nr, nr), nr)
                    return R.at[e, c, p * L + lax.rem(at, L), rows]
                for k in range(1, nz):
                    out.append((piece(s), piece(s), piece(down(s, k, nz)), (g, up(s, k, nz))))
            elif name in ("qxy", "gxy"):
                whole = q_place if name == "qxy" else r_place
                for k in range(1, a):
                    out.append((whole(e, y, x), whole(e, y, x), whole(e, down(y, k, a), x), dev(up(y, k, a), x)))
                for k in range(1, b):
                    out.append((whole(e, y, x), whole(e, y, x), whole(e, y, down(x, k, b)), dev(y, up(x, k, b))))
            elif name in ("qdiag", "gdiag", "fdiag"):
                part = {"qdiag": q_half, "gdiag": r_half, "fdiag": f_half}[name]
                for k in range(1, a):
                    for j in range(1, b):
                        xx = down(x, j, b)
                        out.append((part(e, y, xx, 0), part(e, y, xx, 0), part(e, down(y, k, a), xx, 0), dev(up(y, k, a), x)))
                for k in range(1, a):
                    for j in range(1, b):
                        yy = down(y, k, a)
                        out.append((part(e, yy, x, 1), part(e, yy, x, 1), part(e, yy, down(x, j, b), 1), dev(y, up(x, j, b))))
            elif name == "qback":
                out.append((Q.at[e, c], Q.at[e, c], Q.at[e, oc], core))
            elif name == "gback":
                out.append((R.at[e, c], R.at[e, c], R.at[e, oc], core))
            elif name == "ncore":
                out.append((n_own.at[e], nc_land.at[e], nc_land.at[e], core))
            elif name == "n1":
                for k in range(1, a):
                    out.append((n_chip.at[e], n1_land.at[e, k - 1], n1_land.at[e, k - 1], dev(up(y, k, a), x)))
                for k in range(1, b):
                    at = n1_land.at[e, a - 1 + k - 1]
                    out.append((n_chip.at[e], at, at, dev(y, up(x, k, b))))
            elif name == "n2":
                for k in range(1, b):
                    out.append((n_a.at[e], n2_land.at[e, k - 1], n2_land.at[e, k - 1], dev(y, up(x, k, b))))
                for k in range(1, a):
                    at = n2_land.at[e, b - 1 + k - 1]
                    out.append((n_b.at[e], at, at, dev(up(y, k, a), x)))
            elif name == "nz":
                for k in range(1, nz):
                    out.append((n_place.at[e], nz_land.at[e, k - 1], nz_land.at[e, k - 1], (g, up(s, k, nz))))
            elif name == "rcore":
                out.append((pt.at[e, oc], c_land.at[e], c_land.at[e], core))
            elif name == "p1":
                for k in range(1, a):
                    out.append((cs.at[e, 0, up(y, k, a)], p1a.at[e, k - 1], p1a.at[e, k - 1], dev(up(y, k, a), x)))
                for k in range(1, b):
                    out.append((cs.at[e, 1, :, up(x, k, b)], p1b.at[e, k - 1], p1b.at[e, k - 1], dev(y, up(x, k, b))))
            elif name == "p2":
                for k in range(1, b):
                    out.append((s2a.at[e, up(x, k, b)], p2a.at[e, k - 1], p2a.at[e, k - 1], dev(y, up(x, k, b))))
                for k in range(1, a):
                    out.append((s2b.at[e, up(y, k, a)], p2b.at[e, k - 1], p2b.at[e, k - 1], dev(up(y, k, a), x)))
            elif name == "rz":
                for k in range(1, nz):
                    at = up(s, k, nz)
                    rows = pl.ds(pl.multiple_of((at // L) * nr, nr), nr)
                    out.append((ps.at[e, lax.rem(at, L), rows], z_land.at[e, k - 1], z_land.at[e, k - 1], (g, at)))
            return out

        def q_place(e, yy, xx):
            return Q.at[e, c, yy * b + xx]

        def q_half(e, yy, xx, h):
            return Q.at[e, c, yy * b + xx, pl.ds(h * (nz // 2), nz // 2)]

        def f_place(e, yy, xx):
            return Q.at[e, c, yy * b + xx, s]

        def f_half(e, yy, xx, h):
            return Q.at[e, c, yy * b + xx, s, pl.ds(h * (rb // 2), rb // 2)]

        def r_place(e, yy, xx):
            return R.at[e, c, pl.ds((yy * b + xx) * L, L)]

        def r_half(e, yy, xx, h):
            return R.at[e, c, pl.ds((yy * b + xx) * L + h * L2, L2)]

        def start(name, e):
            for k, (src, dst, _, device) in enumerate(family(name, e)):
                copy(name, e, k, src, dst, device).start()

        def arrived(name, e):
            for k, (src, _, dst, device) in enumerate(family(name, e)):
                copy(name, e, k, src, dst, device).wait_recv()

        def sent(name, e):
            for k, (src, dst, _, device) in enumerate(family(name, e)):
                copy(name, e, k, src, dst, device).wait_send()

        def loads(e):
            at = lax.rem(e, 2)
            return (
                pltpu.make_async_copy(mom.at[e], mom_buf.at[at], load_sem.at[at, 0]),
                pltpu.make_async_copy(grad.at[e], grad_buf.at[at], load_sem.at[at, 1]),
            )

        plan_load = pltpu.make_async_copy(plan_in, plan, plan_sem)
        plan_load.start()
        for e in range(min(2, experts)):
            for one in loads(e):
                one.start()

        barrier = pltpu.get_barrier_semaphore()
        for k in range(1, groups):
            pl.semaphore_signal(barrier, inc=1, device_id=(up(g, k, groups), s), device_id_type=pl.DeviceIdType.MESH)
        for k in range(1, nz):
            pl.semaphore_signal(barrier, inc=1, device_id=(g, up(s, k, nz)), device_id_type=pl.DeviceIdType.MESH)

        def slot_copy(k):
            to = up(g, k, groups)
            return pltpu.make_async_remote_copy(
                src_ref=q_ref.at[:, lax.rem(to, 2), to // 2], dst_ref=slots.at[g],
                send_sem=slot_send.at[k - 1], recv_sem=slot_recv.at[k - 1],
                device_id=(to, s), device_id_type=pl.DeviceIdType.MESH,
            )

        slots[g] = q_ref[:, c, p]
        kept[...] = jnp.zeros_like(kept)
        plan_load.wait()
        pl.semaphore_wait(barrier, groups + nz - 2)
        for k in range(1, groups):
            slot_copy(k).start()
        for k in range(1, groups):
            slot_copy(k).wait_recv()

        @pl.loop(0, experts)
        def _(e):
            own, slot, at = scalar_slot(plan, e, experts, cap)
            factor = jnp.where(slot < plan[experts + own], 1.0, 0.0).astype(F32)
            Q[e, c, p, s] = (slots[own, at].astype(F32) * factor).astype(BF16)

            @pl.when(e < plain)
            def _():
                start("qz", e)

            @pl.when(e >= plain)
            def _():
                start("fxy", e)

        def stage_combine(e):
            for one in loads(e):
                one.wait()
            at = lax.rem(e, 2)
            comb[e] = (mom_buf[at].astype(F32) + grad_buf[at].astype(F32)).astype(BF16)

            @pl.when(e + 2 < experts)
            def _():
                for one in loads(e + 2):
                    one.start()

        def plane_first(before, after):
            @pl.loop(plain, experts)
            def _(e):
                arrived(before, e)
                start(after, e)

        def if_plain(stage):
            def only(e):
                @pl.when(e < plain)
                def _():
                    stage(e)
            return only

        def stage_back(e):
            @pl.when(e < plain)
            def _():
                arrived("qdiag", e)

            @pl.when(e >= plain)
            def _():
                arrived("fz", e)

            start("qback", e)

        def relay(before, after):
            def stage(e):
                arrived(before, e)
                start(after, e)
            return stage

        def merge(parts):
            tot = parts[0]
            for one in parts[1:]:
                tot = tot + one
            scale = lax.rsqrt(tot + stability_offset)
            finite = tot < jnp.inf
            rows = [jnp.where(finite, jnp.sqrt(one + stability_offset) * scale, 0.0) for one in parts]
            rows += [jnp.zeros_like(tot)] * (8 - len(rows))
            weights[...] = jnp.concatenate(rows, axis=0).T
            mine = weights[pl.ds(pl.multiple_of(c * half, half), half), :]
            return tot, [mine[:, k:k + 1] for k in range(len(parts))]

        def stage_left(e):
            arrived("qback", e)
            acc = jnp.zeros((block, rank), F32)
            span = share // 2
            for z in range(nz):
                for h in range(2):
                    rows = Q[e, h, :, z].reshape(span, rank)
                    lo = z * share + h * span
                    acc = acc + jnp.dot(comb[e, :, lo:lo + span], rows, preferred_element_type=F32)
            left_raw[e] = acc
            squares = jnp.sum(acc * acc, axis=0, keepdims=True)
            n_own[e] = squares
            start("ncore", e)
            unit_t = (acc * lax.rsqrt(squares + stability_offset)).T.astype(BF16)
            wide = 2 * LANES
            for j in range(hidden // wide):
                res = jnp.dot(unit_t, comb[e, :, j * wide:(j + 1) * wide], preferred_element_type=F32).astype(BF16)
                for i in range(2):
                    for h in range(2):
                        pt[e, h, 2 * j + i] = res[h * half:(h + 1) * half, i * LANES:(i + 1) * LANES]
            start("rcore", e)

        def stage_chip(e):
            arrived("ncore", e)
            tot, (w_own, w_land) = merge([n_own[e], nc_land[e]])
            n_chip[e] = tot
            start("n1", e)
            arrived("rcore", e)
            for h in range(2):
                for i in range(L2):
                    for pp in range(m):
                        at = pp * L + h * L2 + i
                        cs[e, h, pp // b, pp % b, i] = (
                            pt[e, c, at].astype(F32) * w_own + c_land[e, at].astype(F32) * w_land
                        ).astype(BF16)
            start("p1", e)

        def stage_p1(e):
            arrived("n1", e)
            tot_a, w_a = merge([n_chip[e]] + [n1_land[e, k] for k in range(a - 1)])
            tot_b, w_b = merge([n_chip[e]] + [n1_land[e, a - 1 + k] for k in range(b - 1)])
            n_a[e] = tot_a
            n_b[e] = tot_b
            start("n2", e)
            arrived("p1", e)
            for i in range(b):
                tot = cs[e, 0, y, i].astype(F32) * w_a[0]
                for k in range(a - 1):
                    tot = tot + p1a[e, k, i].astype(F32) * w_a[k + 1]
                s2a[e, i] = tot.astype(BF16)
            for i in range(a):
                tot = cs[e, 1, i, x].astype(F32) * w_b[0]
                for k in range(b - 1):
                    tot = tot + p1b[e, k, i].astype(F32) * w_b[k + 1]
                s2b[e, i] = tot.astype(BF16)
            start("p2", e)

        def stage_p2(e):
            arrived("n2", e)
            tot_a, w_a = merge([n_a[e]] + [n2_land[e, k] for k in range(b - 1)])
            _, w_b = merge([n_b[e]] + [n2_land[e, b - 1 + k] for k in range(a - 1)])
            n_place[e] = tot_a
            start("nz", e)
            arrived("p2", e)
            tot = s2a[e, x].astype(F32) * w_a[0]
            for k in range(b - 1):
                tot = tot + p2a[e, k].astype(F32) * w_a[k + 1]
            ps[e, 0:L2] = tot.astype(BF16)
            tot = s2b[e, y].astype(F32) * w_b[0]
            for k in range(a - 1):
                tot = tot + p2b[e, k].astype(F32) * w_b[k + 1]
            ps[e, L2:L] = tot.astype(BF16)
            start("rz", e)

        def stage_rz(e):
            arrived("nz", e)
            at = pl.multiple_of((s // L) * nr, nr)
            total_squares, w = merge([n_place[e]] + [nz_land[e, k] for k in range(nz - 1)])
            sub = pl.ds(pl.multiple_of(c * half + at, nr), nr)
            w = [weights[sub, k:k + 1] for k in range(nz)]
            arrived("rz", e)
            rows = pl.ds(at, nr)
            tot = ps[e, lax.rem(s, L), rows].astype(F32) * w[0]
            for k in range(nz - 1):
                tot = tot + z_land[e, k].astype(F32) * w[k + 1]
            R[e, c, p * L + lax.rem(s, L), rows] = tot.astype(BF16)
            start("gz", e)
            left[e] = (left_raw[e] * lax.rsqrt(total_squares + stability_offset)).astype(BF16)

        def stage_done(e):
            arrived("gback", e)

            def block_of(i):
                return jnp.concatenate([R[e, 0, i], R[e, 1, i]], axis=0).astype(F32)

            squares = jnp.zeros((rank, LANES), F32)
            for i in range(hb):
                one = block_of(i)
                squares = squares + one * one
            scale = lax.rsqrt(jnp.sum(squares, axis=1, keepdims=True) / hidden + stability_offset)

            unit = left[e]
            for j in range(hb // 2):
                raw = jnp.concatenate([block_of(2 * j), block_of(2 * j + 1)], axis=1)
                span = slice(2 * j * LANES, (2 * j + 2) * LANES)
                low = jnp.dot(unit, raw.astype(BF16), preferred_element_type=F32)
                comb[e, :, span] = (
                    comb[e, :, span].astype(F32) - (1.0 - momentum_decay) * low
                ).astype(BF16)
                new = (raw * scale).astype(BF16)
                upd[e, :, span] = (
                    jnp.dot(unit, new, preferred_element_type=F32) * math.sqrt(D / RANK)
                ).astype(BF16)

            own, slot, _ = scalar_slot(plan, e, experts, cap)
            mine = (slot < plan[experts + own]) & (own == g)
            for i in range(own_blocks):
                new = (block_of(s * own_blocks + i) * scale).astype(BF16).astype(F32)
                for j in range(cap):
                    kept[j, i] += new * jnp.where(mine & (slot == j), 1.0, 0.0).astype(F32)

            special = ("qz", "qxy", "qdiag")
            for name, _ in counts:
                if name[0] != "f" and name not in special:
                    sent(name, e)

            @pl.when(e < plain)
            def _():
                for name in special:
                    sent(name, e)

            @pl.when(e >= plain)
            def _():
                for name in ("fxy", "fdiag", "fz"):
                    sent(name, e)

        stages = [
            (0, if_plain(relay("qz", "qxy"))),
            (2, if_plain(relay("qxy", "qdiag"))),
            (4, stage_back),
            (0, stage_combine),
            (5, stage_left),
            (6, stage_chip),
            (8, stage_p1),
            (10, stage_p2),
            (12, stage_rz),
            (14, relay("gz", "gxy")),
            (16, relay("gxy", "gdiag")),
            (18, relay("gdiag", "gback")),
            (19, stage_done),
        ]

        @pl.loop(0, experts + stages[-1][0])
        def _(t):
            @pl.when(t == 0)
            def _():
                plane_first("fxy", "fdiag")

            @pl.when(t == 1)
            def _():
                plane_first("fdiag", "fz")

            for offset, stage in stages:
                @pl.when((t >= offset) & (t < offset + experts))
                def _():
                    stage(t - offset)

        for j in range(cap):
            for i in range(own_blocks):
                q_out[0, j, i * LANES:(i + 1) * LANES, :] = kept[j, i].T.astype(BF16)
        for k in range(1, groups):
            slot_copy(k).wait_send()

    E = experts
    scratch = [
        pltpu.VMEM((2, block, hidden), BF16),
        pltpu.VMEM((2, block, hidden), BF16),
        pltpu.VMEM((groups, cap, rb, rank), BF16),
        pltpu.VMEM((E, 2, m, nz, rb, rank), BF16),
        pltpu.VMEM((E, block, rank), F32),
        pltpu.VMEM((E, block, rank), BF16),
        pltpu.VMEM((cap, own_blocks, rank, LANES), F32),
        pltpu.VMEM((E, 1, rank), F32),
        pltpu.VMEM((E, 1, rank), F32),
        pltpu.VMEM((E, 1, rank), F32),
        pltpu.VMEM((E, a + b - 2, 1, rank), F32),
        pltpu.VMEM((E, 1, rank), F32),
        pltpu.VMEM((E, 1, rank), F32),
        pltpu.VMEM((E, a + b - 2, 1, rank), F32),
        pltpu.VMEM((E, 1, rank), F32),
        pltpu.VMEM((E, nz - 1, 1, rank), F32),
        pltpu.VMEM((rank, 8), F32),
        pltpu.VMEM((E, 2, hb, half, LANES), BF16),
        pltpu.VMEM((E, hb, half, LANES), BF16),
        pltpu.VMEM((E, 2, a, b, L2, half, LANES), BF16),
        pltpu.VMEM((E, a - 1, b, L2, half, LANES), BF16),
        pltpu.VMEM((E, b - 1, a, L2, half, LANES), BF16),
        pltpu.VMEM((E, b, L2, half, LANES), BF16),
        pltpu.VMEM((E, a, L2, half, LANES), BF16),
        pltpu.VMEM((E, b - 1, L2, half, LANES), BF16),
        pltpu.VMEM((E, a - 1, L2, half, LANES), BF16),
        pltpu.VMEM((E, L, half, LANES), BF16),
        pltpu.VMEM((E, nz - 1, nr, LANES), BF16),
        pltpu.VMEM((E, 2, hb, half, LANES), BF16),
    ]
    outputs = 2 * (2 * E * block * hidden + cap * share * rank)
    limit = min(VMEM_BYTES - outputs, sum(map(vmem_bytes, scratch)) + 11_000_000)
    hbm = pl.BlockSpec(memory_space=pltpu.HBM)
    return pl.pallas_call(
        kernel,
        name="exchange",
        out_shape=(
            jax.ShapeDtypeStruct((E, block, hidden), BF16),
            jax.ShapeDtypeStruct((E, block, hidden), BF16),
            jax.ShapeDtypeStruct((1, cap, share, rank), BF16),
        ),
        in_specs=[hbm, hbm, pl.BlockSpec(memory_space=pltpu.VMEM), hbm],
        out_specs=(pl.BlockSpec(memory_space=pltpu.VMEM),) * 3,
        scratch_shapes=scratch + [
            pltpu.SemaphoreType.DMA((E, total)),
            pltpu.SemaphoreType.DMA((E, total)),
            pltpu.SemaphoreType.DMA((groups - 1,)),
            pltpu.SemaphoreType.DMA((groups - 1,)),
            pltpu.SemaphoreType.DMA((2, 2)),
            pltpu.SMEM(plan_shape, jnp.int32),
            pltpu.SemaphoreType.DMA,
        ],
        compiler_params=pltpu.CompilerParams(
            collective_id=0, has_side_effects=True, vmem_limit_bytes=limit
        ),
    )(momentum, gradient, q_view, plan)


def store(*results):
    pieces = [one.shape[0] for one in results]

    def kernel(*refs):
        n = len(results)
        copies = []
        for at, count in enumerate(pieces):
            for e in range(count):
                copies.append((refs[at].at[e], refs[n + at].at[e]))
        sems = refs[2 * n]
        copies = [pltpu.make_async_copy(a, b, sems.at[k]) for k, (a, b) in enumerate(copies)]
        for one in copies:
            one.start()
        for one in copies:
            one.wait()

    return pl.pallas_call(
        kernel,
        name="store",
        out_shape=tuple(jax.ShapeDtypeStruct(one.shape, one.dtype) for one in results),
        in_specs=[pl.BlockSpec(memory_space=pltpu.VMEM)] * len(results),
        out_specs=(pl.BlockSpec(memory_space=pltpu.HBM),) * len(results),
        scratch_shapes=[pltpu.SemaphoreType.DMA((sum(pieces),))],
        compiler_params=pltpu.CompilerParams(vmem_limit_bytes=24_000_000),
    )(*results)


def shards(momentum, gradient, q_prev, owner_group, group_counts):
    plan = jnp.concatenate([owner_group, group_counts])
    return store(*exchange(momentum, gradient, q_prev, plan))


def solution(mesh):
    return jax.shard_map(
        shards,
        mesh=mesh,
        in_specs=(
            P(None, AXES, None),
            P(None, AXES, None),
            P("group", None, "shard", None),
            P(),
            P(),
        ),
        out_specs=(P(None, AXES, None), P(None, AXES, None), P("group", None, "shard", None)),
        check_vma=False,
    )
```
